256 devices in a mesh: band: 32 (over z, x_hi, core), lane: 8 (over y, x_lo).
Axes of the slice: x: 4 (x_hi: 2, x_lo: 2; x = x_hi * 2 + x_lo), y: 4, z: 8, core: 2. Of those that a mesh axis runs over, the one named last changes fastest.
Arguments:
- load_terms: float32 [2048, 512, 256], P('band', 'lane'), may hold values from -6 to 6
- start_values: float32 [2048, 512, 256], P('band', 'lane'), may hold values from -6 to 6
- reaction_rate: float32 [2048, 512, 256], P('band', 'lane'), may hold values from 0.1 to 0.9
Outputs:
- solution: float32 [2048, 512, 256], P('band', 'lane')
- remaining: float32 [2048, 512, 256], P('band', 'lane')
The draws below stay inside these ranges and needn't reach their ends.
All inputs are finite; a program needn't handle non-finite values.
Results may differ from the reference program's by a relative error of at most 0.0003.
Values sent between devices are 32-bit elements.
No kernel may reach another device: no remote copies, remote signals or barrier semaphores. Data moves between devices by JAX's collectives and lax.ppermute only.
A program may use at most 128 MiB of HBM per device.

```python
import jax
import jax.numpy as jnp
from jax import lax

LAYERS = 256
RATIO = 2
BEFORE = 3
AFTER = 2
INNER = 13
GRID_Y = 2048
GRID_X = 512


def levels(key, dims, shards, smallest, high):
    factor_of, own = 1.0, jax.random.fold_in(key, 6)
    for axis_at, shards_of in shards:
        steps = jnp.exp(jax.random.uniform(jax.random.fold_in(own, axis_at), (shards_of,), jnp.float32, smallest / len(shards), high / len(shards)))
        factor_of = factor_of * jnp.repeat(steps, dims[axis_at] // shards_of).reshape([-1 if axis == axis_at else 1 for axis in range(len(dims))])
    return factor_of


def gaussian(own_key, shape, width, bound, cuts=(), kind=jnp.bfloat16):
    level = levels(own_key, shape, cuts, -0.22, 0.18) if cuts else 1.0
    entries = jax.random.normal(own_key, shape, jnp.float32) * width * level
    return jnp.minimum(jnp.maximum(entries, -bound), bound).astype(kind)


def setup_inputs(seed: int = 0) -> dict:
    seeds = jax.random.split(jax.random.key(seed), 4)
    load_terms = gaussian(seeds[0], (GRID_Y, GRID_X, LAYERS), 1.0, 6.0, ((0, 32), (1, 8)), jnp.float32)
    start_values = gaussian(seeds[1], (GRID_Y, GRID_X, LAYERS), 1.0, 6.0, ((0, 32), (1, 8)), jnp.float32)
    reaction_rate = jnp.clip(0.1 + 0.79999997 * jax.random.uniform(seeds[2], (GRID_Y, GRID_X, LAYERS), jnp.float32) ** levels(seeds[2], (GRID_Y, GRID_X, LAYERS), ((0, 32), (1, 8)), -0.2, 0.2), 0.1, 0.9)
    return dict(load_terms=load_terms, start_values=start_values, reaction_rate=reaction_rate)


def cross_sum(padded):
    inner_y, inner_x = padded.shape[0] - 2, padded.shape[1] - 2
    middle_rows = lax.slice_in_dim(padded, 1, 1 + inner_y, axis=0)
    middle_columns = lax.slice_in_dim(padded, 1, 1 + inner_x, axis=1)
    return (lax.slice_in_dim(middle_columns, 0, inner_y, axis=0) + lax.slice_in_dim(middle_columns, 2, 2 + inner_y, axis=0)
            + lax.slice_in_dim(middle_rows, 0, inner_x, axis=1) + lax.slice_in_dim(middle_rows, 2, 2 + inner_x, axis=1))


def smooth_step(padded, values, load, mass_here):
    return values + 0.8 * (load + cross_sum(padded) - (4.0 + mass_here) * values) / (4.0 + mass_here)


def block_means(values):
    cut = values.reshape(values.shape[0] // RATIO, RATIO, values.shape[1] // RATIO, RATIO, values.shape[2])
    return jnp.mean(cut, axis=(1, 3))


def spread_blocks(values):
    return jnp.repeat(jnp.repeat(values, RATIO, axis=0), RATIO, axis=1)


def reference(load_terms, start_values, reaction_rate):
    values = start_values
    for sweep in range(BEFORE):
        values = smooth_step(jnp.pad(values, ((1, 1), (1, 1), (0, 0)), mode="constant"), values, load_terms, reaction_rate)
    defect = load_terms + cross_sum(jnp.pad(values, ((1, 1), (1, 1), (0, 0)), mode="constant")) - (4.0 + reaction_rate) * values
    coarse_load, coarse_mass = block_means(defect) * RATIO, block_means(reaction_rate) * RATIO
    coarse_values = jnp.zeros_like(coarse_load)
    for sweep in range(INNER):
        coarse_values = smooth_step(jnp.pad(coarse_values, ((1, 1), (1, 1), (0, 0)), mode="constant"), coarse_values, coarse_load, coarse_mass)
    values = values + spread_blocks(coarse_values)
    for sweep in range(AFTER):
        values = smooth_step(jnp.pad(values, ((1, 1), (1, 1), (0, 0)), mode="constant"), values, load_terms, reaction_rate)
    solution = values
    remaining = load_terms + cross_sum(jnp.pad(solution, ((1, 1), (1, 1), (0, 0)), mode="constant")) - (4.0 + reaction_rate) * solution
    return solution, remaining
```

```python
import functools

import jax
import jax.numpy as jnp
from jax import lax
from jax.experimental import pallas as pl
from jax.experimental.pallas import tpu as pltpu
from jax.sharding import PartitionSpec as P

LANES = 128
CHAINS = 1
INNER = 13
FINE = 4
TILE = 8
DEEP = 8
SECOND = 6
FIRST_SWEEPS = DEEP + 1
LAST_SWEEPS = INNER - FIRST_SWEEPS


def swaps(count, first):
    pairs = []
    for i in range(first, count - 1, 2):
        pairs += [(i, i + 1), (i + 1, i)]
    return pairs


def swap(axis, even, odd):
    count = lax.axis_size(axis)
    return (
        lax.ppermute(even, axis, swaps(count, 0)),
        lax.ppermute(odd, axis, swaps(count, 1)),
    )


def placement():
    words = []
    for axis in ("band", "lane"):
        at, count = lax.axis_index(axis), lax.axis_size(axis)
        words += [at % 2 == 0, at > 0, at < count - 1]
    return jnp.stack([w.astype(jnp.int32) for w in words])


def roll(value, shift, axis):
    return pltpu.roll(value, shift % value.shape[axis], axis)


def sublane(value):
    return lax.broadcasted_iota(jnp.int32, value.shape, value.ndim - 2)


def by_side(even, got_even, got_odd):
    low = jnp.where(even, got_odd, got_even)
    high = jnp.where(even, got_even, got_odd)
    return low, high


def weight(mass, inside):
    return jnp.where(inside, 0.8 / (4.0 + mass), 0.0)


def new_value(here, left, right, up, down, load, w):
    return 0.2 * here + w * (load + ((up + down) + (left + right)))


def lane_pack_kernel(
    place, u_first, f_first, m_first, u_last, f_last, m_last, got_e, got_o, even_ref, odd_ref
):
    even_b, low_b, high_b = place[0] == 1, place[1] == 1, place[2] == 1
    even_l = place[3] == 1
    rows = u_first.shape[0]

    def message(u_ref, f_ref, m_ref, tile, high):
        at = pl.ds(tile * TILE, TILE)
        low_rows, high_rows = by_side(even_b, got_e[:, at, :], got_o[:, at, :])
        zero = jnp.zeros((1,) + u_ref.shape[1:], jnp.float32)
        u = jnp.concatenate([low_rows[:4], u_ref[...], high_rows[:4]], axis=0)
        f = jnp.concatenate([zero, low_rows[4:7], f_ref[...], high_rows[4:7], zero], axis=0)
        m = jnp.concatenate([zero, low_rows[7:10], m_ref[...], high_rows[7:10], zero], axis=0)
        w = 0.8 / (4.0 + m)
        w = jnp.concatenate(
            [
                jnp.where(low_b, w[:4], 0.0),
                w[4 : 4 + rows],
                jnp.where(high_b, w[4 + rows :], 0.0),
            ],
            axis=0,
        )
        up = jnp.concatenate([zero, u[:-1]], axis=0)
        down = jnp.concatenate([u[1:], zero], axis=0)
        v = new_value(u, roll(u, 1, 1), roll(u, -1, 1), up, down, f, w)
        s = sublane(u)
        if high:
            return jnp.where(
                s >= 6, u, jnp.where(s >= 4, roll(v, -1, 1), jnp.where(s >= 2, roll(f, -4, 1), roll(m, -6, 1)))
            )
        return jnp.where(
            s < 2, u, jnp.where(s < 4, roll(v, 1, 1), jnp.where(s < 6, roll(f, 4, 1), roll(m, 6, 1)))
        )

    last_tile = got_e.shape[1] // TILE - 1
    low = message(u_first, f_first, m_first, 0, False)
    high = message(u_last, f_last, m_last, last_tile, True)
    even_ref[...] = jnp.where(even_l, high, low)
    odd_ref[...] = jnp.where(even_l, low, high)


def fine_fields(place, f_ref, m_ref, got_e, got_o, lane_e, lane_o, load, w):
    even_b, low_b, high_b = place[0] == 1, place[1] == 1, place[2] == 1
    even_l, low_l, high_l = place[3] == 1, place[4] == 1, place[5] == 1
    rows, columns = f_ref.shape[0], f_ref.shape[1]
    own = pl.ds(TILE, columns)

    def copy_row(r, _):
        load[FINE + r, own, :] = f_ref[r]
        w[FINE + r, own, :] = 0.8 / (4.0 + m_ref[r])
        return 0

    lax.fori_loop(0, rows, copy_row, 0, unroll=2)
    low_rows, high_rows = by_side(even_b, got_e[4:10], got_o[4:10])
    load[1:4, own, :] = low_rows[:3]
    w[1:4, own, :] = weight(low_rows[3:], low_b)
    load[pl.ds(FINE + rows, 3), own, :] = high_rows[:3]
    w[pl.ds(FINE + rows, 3), own, :] = weight(high_rows[3:], high_b)

    def lane_row(r, _):
        low, high = by_side(even_l, lane_e[r], lane_o[r])
        s = sublane(low)
        inside_row = ((r >= FINE) | low_b) & ((r < FINE + rows) | high_b)
        load[r, pl.ds(0, TILE), :] = roll(low, 4, 0)
        load[r, pl.ds(TILE + columns, TILE), :] = roll(high, -4, 0)
        w[r, pl.ds(0, TILE), :] = weight(roll(low, 6, 0), (s >= 6) & inside_row & low_l)
        w[r, pl.ds(TILE + columns, TILE), :] = weight(
            roll(high, -6, 0), (s < 2) & inside_row & high_l
        )
        return 0

    lax.fori_loop(0, rows + 2 * FINE, lane_row, 0, unroll=4)


def sweep(source, target, load, w, first, last):
    def row(r, carry):
        up, here = carry
        down = source[r + 1]
        target[r] = new_value(here, roll(here, 1, 0), roll(here, -1, 0), up, down, load[r], w[r])
        return here, down

    lax.fori_loop(first, last, row, (source[first - 1], source[first]), unroll=2)


def before_kernel(
    place, u_ref, f_ref, m_ref, got_e, got_o, lane_e, lane_o,
    v_ref, load_ref, mass_ref, a, b, load, w, pairs,
):
    even_b, even_l = place[0] == 1, place[3] == 1
    rows, columns = u_ref.shape[0], u_ref.shape[1]
    own, left, right = pl.ds(TILE, columns), pl.ds(0, TILE), pl.ds(TILE + columns, TILE)
    fine_fields(place, f_ref, m_ref, got_e, got_o, lane_e, lane_o, load, w)
    low_rows, high_rows = by_side(even_b, got_e[:4], got_o[:4])
    a[:4, own, :] = low_rows
    a[pl.ds(FINE + rows, 4), own, :] = high_rows

    def copy_row(r, _):
        a[FINE + r, own, :] = u_ref[r]
        return 0

    lax.fori_loop(0, rows, copy_row, 0, unroll=4)

    def lane_row(r, _):
        low, high = by_side(even_l, lane_e[r], lane_o[r])
        a[r, left, :] = low
        a[r, right, :] = high
        return 0

    lax.fori_loop(0, rows + 2 * FINE, lane_row, 0, unroll=4)
    end = rows + 2 * FINE
    sweep(a, b, load, w, 1, end - 1)

    def mend(r, _):
        low, high = by_side(even_l, lane_e[r], lane_o[r])
        s = sublane(low)
        b[r, left, :] = jnp.where(s == 7, b[r, left, :], roll(low, 1, 0))
        b[r, right, :] = jnp.where(s == 0, b[r, right, :], roll(high, -1, 0))
        return 0

    lax.fori_loop(1, end - 1, mend, 0, unroll=2)
    sweep(b, a, load, w, 2, end - 2)
    sweep(a, b, load, w, 3, end - 3)

    def defect_of(i, up, here, down):
        around = (up + down) + (roll(here, 1, 0) + roll(here, -1, 0))
        value = lax.slice_in_dim(load[FINE + i] + around, TILE, TILE + columns, axis=0)
        mine = lax.slice_in_dim(here, TILE, TILE + columns, axis=0)
        return mine, value - (4.0 + m_ref[i]) * mine

    even_columns, odd_columns = pl.ds(0, columns // 2, 2), pl.ds(1, columns // 2, 2)

    def restrict(k, carry):
        up, here = carry
        i = 2 * k
        middle, down = b[FINE + i + 1], b[FINE + i + 2]
        mine, first = defect_of(i, up, here, middle)
        v_ref[i] = mine
        mine, second = defect_of(i + 1, here, middle, down)
        v_ref[i + 1] = mine
        pairs[0, k] = first + second
        pairs[1, k] = m_ref[i] + m_ref[i + 1]
        load_ref[k] = 0.5 * (pairs[0, k, even_columns, :] + pairs[0, k, odd_columns, :])
        mass_ref[k] = 0.5 * (pairs[1, k, even_columns, :] + pairs[1, k, odd_columns, :])
        return middle, down

    lax.fori_loop(0, rows // 2, restrict, (b[FINE - 1], b[FINE]))


def coarse_pack_kernel(
    place, load_first, mass_first, v_first, load_last, mass_last, v_last, got_e, got_o,
    even_ref, odd_ref,
):
    even_b, even_l = place[0] == 1, place[3] == 1
    half = got_e.shape[1]
    zero = jnp.zeros((1, TILE, LANES), jnp.float32)

    def message(load_ref, mass_ref, v_ref, high):
        coarse_at = pl.ds(half - TILE if high else 0, TILE)
        low, top = by_side(even_b, got_e[: 2 * DEEP, coarse_at, :], got_o[: 2 * DEEP, coarse_at, :])
        load = jnp.concatenate([low[:DEEP], load_ref[...], top[:DEEP]], axis=0)
        mass = jnp.concatenate([low[DEEP:], mass_ref[...], top[DEEP:]], axis=0)
        fine_at = pl.ds(half - TILE if high else 0, TILE)
        rows_e = [got_e[2 * DEEP + 2 * i + (1 if high else 0), fine_at, :][None] for i in range(3)]
        rows_o = [got_o[2 * DEEP + 2 * i + (1 if high else 0), fine_at, :][None] for i in range(3)]
        low_v, top_v = by_side(
            even_b, jnp.concatenate(rows_e, axis=0), jnp.concatenate(rows_o, axis=0)
        )
        v = jnp.concatenate([zero, low_v, v_ref[...], top_v, zero], axis=0)
        split = v.shape[0] // 2
        s = sublane(v[:split])
        keep = s >= 4 if high else s < 4
        return jnp.concatenate([load, mass, jnp.where(keep, v[:split], roll(v[split:], 4, 1))], axis=0)

    low = message(load_first, mass_first, v_first, False)
    high = message(load_last, mass_last, v_last, True)
    even_ref[...] = jnp.where(even_l, high, low)
    odd_ref[...] = jnp.where(even_l, low, high)


def coarse_fields(place, load_ref, mass_ref, got_e, got_o, lane_e, lane_o, load, w):
    even_b, low_b, high_b = place[0] == 1, place[1] == 1, place[2] == 1
    even_l, low_l, high_l = place[3] == 1, place[4] == 1, place[5] == 1
    rows, columns = load_ref.shape[0], load_ref.shape[1]
    own = pl.ds(TILE, columns)

    def copy_row(r, _):
        load[DEEP + r, own, :] = load_ref[r]
        w[DEEP + r, own, :] = 0.8 / (4.0 + mass_ref[r])
        return 0

    lax.fori_loop(0, rows, copy_row, 0, unroll=4)
    low, high = by_side(even_b, got_e[: 2 * DEEP], got_o[: 2 * DEEP])
    load[:DEEP, own, :] = low[:DEEP]
    w[:DEEP, own, :] = weight(low[DEEP:], low_b)
    load[pl.ds(DEEP + rows, DEEP), own, :] = high[:DEEP]
    w[pl.ds(DEEP + rows, DEEP), own, :] = weight(high[DEEP:], high_b)
    total = rows + 2 * DEEP

    def lane_row(r, _):
        inside_row = ((r >= DEEP) | low_b) & ((r < DEEP + rows) | high_b)
        low, high = by_side(even_l, lane_e[r], lane_o[r])
        load[r, pl.ds(0, TILE), :] = low
        load[r, pl.ds(TILE + columns, TILE), :] = high
        low, high = by_side(even_l, lane_e[total + r], lane_o[total + r])
        w[r, pl.ds(0, TILE), :] = weight(low, inside_row & low_l)
        w[r, pl.ds(TILE + columns, TILE), :] = weight(high, inside_row & high_l)
        return 0

    lax.fori_loop(0, total, lane_row, 0, unroll=4)


def coarse_kernel(
    place, load_ref, mass_ref, got_e, got_o, lane_e, lane_o, x_ref, a, b, load, w
):
    rows, columns = load_ref.shape[0], load_ref.shape[1]
    coarse_fields(place, load_ref, mass_ref, got_e, got_o, lane_e, lane_o, load, w)
    total = rows + 2 * DEEP

    def first(r, _):
        a[r] = w[r] * load[r]
        return 0

    lax.fori_loop(0, total, first, 0, unroll=4)
    source, target = a, b
    for step in range(1, FIRST_SWEEPS):
        sweep(source, target, load, w, step, total - step)
        source, target = target, source

    def out(r, _):
        x_ref[r] = source[DEEP + r, pl.ds(TILE, columns), :]
        return 0

    lax.fori_loop(0, rows, out, 0, unroll=4)


def value_pack_kernel(place, x_first, x_last, got_e, got_o, even_ref, odd_ref):
    even_b, even_l = place[0] == 1, place[3] == 1
    last = got_e.shape[1] - TILE

    def message(x_ref, start):
        at = pl.ds(start, TILE)
        low, high = by_side(even_b, got_e[:, at, :], got_o[:, at, :])
        return jnp.concatenate([low, x_ref[...], high], axis=0)

    low, high = message(x_first, 0), message(x_last, last)
    even_ref[...] = jnp.where(even_l, high, low)
    odd_ref[...] = jnp.where(even_l, low, high)


def after_kernel(
    place, f_ref, m_ref, v_ref, load_ref, mass_ref, x_ref,
    fine_e, fine_o, fine_lane_e, fine_lane_o,
    coarse_e, coarse_o, coarse_lane_e, coarse_lane_o,
    value_e, value_o, value_lane_e, value_lane_o,
    *rest,
):
    u_ref, d_ref, a, b, load, w, x, y, coarse_load, coarse_w, spread = rest[-11:]
    even_b, even_l = place[0] == 1, place[3] == 1
    rows, columns = f_ref.shape[0], f_ref.shape[1]
    half_rows, half_columns = rows // 2, columns // 2
    coarse_fields(
        place, load_ref, mass_ref, coarse_e, coarse_o, coarse_lane_e, coarse_lane_o, coarse_load, coarse_w
    )
    own = pl.ds(TILE, half_columns)
    total = half_rows + 2 * DEEP
    low, high = by_side(even_b, value_e[...], value_o[...])
    x[DEEP - SECOND : DEEP, own, :] = low
    x[pl.ds(DEEP + half_rows, SECOND), own, :] = high

    def coarse_copy(r, _):
        x[DEEP + r, own, :] = x_ref[r]
        return 0

    lax.fori_loop(0, half_rows, coarse_copy, 0, unroll=4)

    def coarse_lane(r, _):
        low, high = by_side(even_l, value_lane_e[r], value_lane_o[r])
        x[DEEP - SECOND + r, pl.ds(0, TILE), :] = low
        x[DEEP - SECOND + r, pl.ds(TILE + half_columns, TILE), :] = high
        return 0

    lax.fori_loop(0, half_rows + 2 * SECOND, coarse_lane, 0, unroll=4)
    source, target = x, y
    for step in range(1, LAST_SWEEPS + 1):
        edge = DEEP - SECOND + step
        sweep(source, target, coarse_load, coarse_w, edge, total - edge)
        source, target = target, source

    fine_fields(place, f_ref, m_ref, fine_e, fine_o, fine_lane_e, fine_lane_o, load, w)

    fine_own, left, right = pl.ds(TILE, columns), pl.ds(0, TILE), pl.ds(TILE + columns, TILE)
    for i in range(3):
        for part in range(2):
            at = pl.ds(TILE + part * half_columns, half_columns)
            k = 2 * DEEP + 2 * i + part
            low, high = by_side(even_b, coarse_e[k], coarse_o[k])
            a[1 + i, at, :] = low
            a[FINE + rows + i, at, :] = high

    def fine_copy(r, _):
        a[FINE + r, fine_own, :] = v_ref[r]
        return 0

    lax.fori_loop(0, rows, fine_copy, 0, unroll=4)
    split = (rows + 2 * FINE) // 2

    def fine_lane(r, _):
        low, high = by_side(even_l, coarse_lane_e[2 * total + r], coarse_lane_o[2 * total + r])
        a[r, left, :] = low
        a[r, right, :] = high
        a[split + r, left, :] = roll(low, 4, 0)
        a[split + r, right, :] = roll(high, 4, 0)
        return 0

    lax.fori_loop(0, split, fine_lane, 0, unroll=4)

    wide = columns + 2 * TILE
    across = wide // 2
    skip = TILE - TILE // 2

    def correct(k, _):
        value = source[DEEP - 2 + k, pl.ds(skip, across), :]
        spread[k, pl.ds(0, across, 2), :] = value
        spread[k, pl.ds(1, across, 2), :] = value
        both = spread[k]
        a[2 * k] += both
        a[2 * k + 1] += both
        return 0

    lax.fori_loop(0, half_rows + 4, correct, 0, unroll=2)
    end = rows + 2 * FINE
    sweep(a, b, load, w, 2, end - 2)
    sweep(b, a, load, w, 3, end - 3)

    def remains(i, carry):
        up, here = carry
        down = a[FINE + i + 1]
        around = (up + down) + (roll(here, 1, 0) + roll(here, -1, 0))
        value = lax.slice_in_dim(load[FINE + i] + around, TILE, TILE + columns, axis=0)
        mine = lax.slice_in_dim(here, TILE, TILE + columns, axis=0)
        u_ref[i] = mine
        d_ref[i] = value - (4.0 + m_ref[i]) * mine
        return here, down

    lax.fori_loop(0, rows, remains, (a[FINE - 1], a[FINE]), unroll=2)


def call(kernel, outs, ins, args, lanes, scratch=(), aliases=None, interpret=False):
    def spec(entry):
        if entry is None:
            return pl.BlockSpec(memory_space=pl.ANY)
        shape, at, start = entry
        return pl.BlockSpec(shape + (LANES,), lambda i, at=at, start=start: at + (i + start,))

    return pl.pallas_call(
        kernel,
        grid=(lanes // LANES,),
        in_specs=[pl.BlockSpec(memory_space=pltpu.SMEM)] + [spec(e) for e in ins],
        out_specs=[spec(e) for e, _ in outs],
        out_shape=[jax.ShapeDtypeStruct(s, jnp.float32) for _, s in outs],
        scratch_shapes=[pltpu.VMEM(s + (LANES,), jnp.float32) for s in scratch],
        input_output_aliases=aliases or {},
        interpret=interpret,
        compiler_params=pltpu.CompilerParams(vmem_limit_bytes=60 * 1024 * 1024),
    )(*args)


def edge(value, even, depth):
    rows = value.shape[0]
    high = jnp.where(even, rows - depth, 0)
    low = jnp.where(even, 0, rows - depth)
    return (
        lax.dynamic_slice_in_dim(value, high, depth, axis=0),
        lax.dynamic_slice_in_dim(value, low, depth, axis=0),
    )


def joined(parts, even):
    strips = [edge(value, even, depth) for value, depth in parts]
    return tuple(jnp.concatenate([s[k] for s in strips], axis=0) for k in range(2))


def body(load_terms, start_values, reaction_rate, interpret=False):
    run = functools.partial(call, interpret=interpret)
    place = placement()
    even = lax.axis_index("band") % 2 == 0
    rows, columns, layers = load_terms.shape
    half_rows, half_columns = rows // 2, columns // 2
    lanes = layers // CHAINS
    blocks = lanes // LANES
    end = rows + 2 * FINE
    total = half_rows + 2 * DEEP
    wide = columns + 2 * TILE
    half_wide = half_columns + 2 * TILE
    last = columns // TILE - 1
    half_last = half_columns // TILE - 1
    outputs = ()
    for chain in range(CHAINS):
        start = chain * blocks

        def cut(value):
            return lax.slice_in_dim(value, chain * lanes, (chain + 1) * lanes, axis=2)

        u, f, m = start_values, load_terms, reaction_rate
        fine = swap("band", *joined([(cut(u), 4), (cut(f), 3), (cut(m), 3)], even))
        fine_spec = [((10, columns), (0, 0), 0)] * 2
        whole = ((rows, columns), (0, 0), start)
        first_tile, last_tile = ((rows, TILE), (0, 0), start), ((rows, TILE), (0, last), start)
        lane_spec = [((end, TILE), (0, 0), 0)] * 2
        fine_lane = run(
            lane_pack_kernel,
            [(e, (end, TILE, lanes)) for e in lane_spec],
            [first_tile] * 3 + [last_tile] * 3 + fine_spec,
            (place, u, f, m, u, f, m, *fine),
            lanes,
        )
        fine_lane = swap("lane", *fine_lane)
        coarse_block = ((half_rows, half_columns), (0, 0), 0)
        own_block = ((rows, columns), (0, 0), 0)
        v, load, mass = run(
            before_kernel,
            [
                (own_block, (rows, columns, lanes)),
                (coarse_block, (half_rows, half_columns, lanes)),
                (coarse_block, (half_rows, half_columns, lanes)),
            ],
            [whole] * 3 + fine_spec + lane_spec,
            (place, u, f, m, *fine, *fine_lane),
            lanes,
            scratch=[(end, wide)] * 4 + [(2, half_rows, columns)],
        )
        strips = joined([(load, DEEP), (mass, DEEP)], even)
        values = [s.reshape(6, half_columns, lanes) for s in edge(v, even, 3)]
        coarse = swap("band", *[jnp.concatenate([s, t], axis=0) for s, t in zip(strips, values)])
        coarse_spec = [((2 * DEEP + 6, half_columns), (0, 0), 0)] * 2
        lane_rows = 2 * total + end // 2
        coarse_lane_spec = [((lane_rows, TILE), (0, 0), 0)] * 2
        half_first = ((half_rows, TILE), (0, 0), 0)
        half_last_tile = ((half_rows, TILE), (0, half_last), 0)
        coarse_lane = run(
            coarse_pack_kernel,
            [(e, (lane_rows, TILE, lanes)) for e in coarse_lane_spec],
            [half_first, half_first, ((rows, TILE), (0, 0), 0)]
            + [half_last_tile, half_last_tile, ((rows, TILE), (0, last), 0)]
            + coarse_spec,
            (place, load, mass, v, load, mass, v, *coarse),
            lanes,
        )
        coarse_lane = swap("lane", *coarse_lane)
        (x,) = run(
            coarse_kernel,
            [(coarse_block, (half_rows, half_columns, lanes))],
            [coarse_block] * 2 + coarse_spec + coarse_lane_spec,
            (place, load, mass, *coarse, *coarse_lane),
            lanes,
            scratch=[(total, half_wide)] * 4,
        )
        value = swap("band", *edge(x, even, SECOND))
        value_spec = [((SECOND, half_columns), (0, 0), 0)] * 2
        value_rows = half_rows + 2 * SECOND
        value_lane_spec = [((value_rows, TILE), (0, 0), 0)] * 2
        value_lane = run(
            value_pack_kernel,
            [(e, (value_rows, TILE, lanes)) for e in value_lane_spec],
            [half_first, half_last_tile] + value_spec,
            (place, x, x, *value),
            lanes,
        )
        value_lane = swap("lane", *value_lane)
        args = (
            place, f, m, v, load, mass, x, *fine, *fine_lane, *coarse, *coarse_lane, *value, *value_lane,
        )
        ins = (
            [whole] * 2
            + [own_block]
            + [coarse_block] * 3
            + fine_spec
            + lane_spec
            + coarse_spec
            + coarse_lane_spec
            + value_spec
            + value_lane_spec
        )
        outputs = run(
            after_kernel,
            [(whole, (rows, columns, layers))] * 2,
            ins + [None] * len(outputs),
            args + tuple(outputs),
            lanes,
            scratch=[(end, wide)] * 4 + [(total, half_wide)] * 4 + [(half_rows + 4, wide)],
            aliases={len(args) + k: k for k in range(len(outputs))},
        )
    return tuple(outputs)


def solution(mesh):
    return jax.shard_map(
        body,
        mesh=mesh,
        in_specs=(P("band", "lane", None), P("band", "lane", None), P("band", "lane", None)),
        out_specs=(P("band", "lane", None), P("band", "lane", None)),
        check_vma=False,
    )
```

```python
import functools

import jax
import jax.numpy as jnp
from jax import lax
from jax.experimental import pallas as pl
from jax.experimental.pallas import tpu as pltpu
from jax.sharding import PartitionSpec as P

LANES = 128
INNER = 13
FINE = 4
TILE = 8
DEEP = 8
SECOND = 6
FIRST_SWEEPS = DEEP + 1
LAST_SWEEPS = INNER - FIRST_SWEEPS
CHUNKS = 4
FAR = 60
MASS = 56
NEAR = 55
BEFORE = 48
AFTER = 46
COST = 500_000_000


def swaps(count, first):
    pairs = []
    for i in range(first, count - 1, 2):
        pairs += [(i, i + 1), (i + 1, i)]
    return pairs


def swap(axis, even, odd):
    count = lax.axis_size(axis)
    return (
        lax.ppermute(even, axis, swaps(count, 0)),
        lax.ppermute(odd, axis, swaps(count, 1)),
    )


def place(axis):
    at, count = lax.axis_index(axis), lax.axis_size(axis)
    return lax.rem(at, 2) == 0, at > 0, at < count - 1


def roll(value, shift, axis):
    return pltpu.roll(value, shift % value.shape[axis], axis)


def sublane(value):
    return lax.broadcasted_iota(jnp.int32, value.shape, value.ndim - 2)


def by_side(even, got_even, got_odd):
    low = jnp.where(even, got_odd, got_even)
    high = jnp.where(even, got_even, got_odd)
    return low, high


def weight(mass, inside):
    return jnp.where(inside, 0.8 / (4.0 + mass), 0.0)


def new_value(here, left, right, up, down, load, w):
    return 0.2 * here + w * (load + ((up + down) + (left + right)))


def edges(even, rows, depth):
    return jnp.where(even, rows - depth, 0), jnp.where(even, 0, rows - depth)


def first_kernel(chain, u_hbm, f_hbm, m_hbm, even_ref, odd_ref, sems):
    even_b, _, _ = place("band")
    rows = m_hbm.shape[0]
    layers = pl.ds(chain * LANES, LANES)
    copies = []
    for side, target in enumerate((even_ref, odd_ref)):
        for part, (hbm, depth, at) in enumerate(((u_hbm, 4, 0), (f_hbm, 3, 4), (m_hbm, 3, 7))):
            start = edges(even_b, rows, depth)[side]
            copy = pltpu.make_async_copy(
                hbm.at[pl.ds(start, depth), :, layers],
                target.at[pl.ds(at, depth)],
                sems.at[3 * side + part],
            )
            copy.start()
            copies.append(copy)
    for copy in copies:
        copy.wait()


def mass_kernel(chain, m_hbm, mass_ref, even_ref, odd_ref, m_own, pairs, sems):
    even_b, _, _ = place("band")
    groups, rows, columns = m_own.shape[0], m_own.shape[1], m_own.shape[2]
    copies = []
    for g in range(groups):
        copy = pltpu.make_async_copy(m_hbm.at[:, :, pl.ds(g * LANES, LANES)], m_own.at[g], sems.at[g])
        copy.start()
        copies.append(copy)
    even_columns, odd_columns = pl.ds(0, columns // 2, 2), pl.ds(1, columns // 2, 2)
    for g in range(groups):
        copies[g].wait()

        def restrict(k, _, g=g):
            pairs[k] = m_own[g, 2 * k] + m_own[g, 2 * k + 1]
            mass_ref[g, k] = 0.5 * (pairs[k, even_columns, :] + pairs[k, odd_columns, :])
            return 0

        lax.fori_loop(0, rows // 2, restrict, 0, unroll=2)
        for side, target in enumerate((even_ref, odd_ref)):
            start = edges(even_b, rows // 2, DEEP)[side]
            target[g] = mass_ref[g, pl.ds(start, DEEP)]


def fold(value, side):
    rows, depth = value.shape[0] - 2 * DEEP, DEEP
    s = sublane(value[0])
    merged = []
    for r in range(1, depth):
        other = value[depth + rows - 1 + r]
        if side:
            merged.append(jnp.where(s >= depth - r, value[r], roll(other, -r, 0))[None])
        else:
            merged.append(jnp.where(s < r, value[r], roll(other, r, 0))[None])
    return jnp.concatenate(merged + [value[depth : depth + rows]], axis=0)


def unfold(got_e, got_o, even, rows, write, first=0):
    def own(k, _):
        low, high = by_side(even, got_e(first + DEEP - 1 + k), got_o(first + DEEP - 1 + k))
        write(DEEP + k, low, high)
        return 0

    lax.fori_loop(0, rows, own, 0, unroll=4)
    for r in range(1, DEEP):
        low, high = by_side(even, got_e(first + r - 1), got_o(first + r - 1))
        write(r, low, high)
        write(DEEP + rows - 1 + r, roll(low, r, 0), roll(high, -r, 0))


def mass_pack_kernel(chain, mass_ref, got_e, got_o, even_ref, odd_ref):
    even_b, even_l = place("band")[0], place("lane")[0]
    half = mass_ref.shape[2]
    for g in range(mass_ref.shape[0]):

        def message(side, g=g):
            at = pl.ds(side * (half - TILE), TILE)
            low, high = by_side(even_b, got_e[g, :, at, :], got_o[g, :, at, :])
            return fold(jnp.concatenate([low, mass_ref[g, :, at, :], high], axis=0), side)

        low, high = message(0), message(1)
        even_ref[g] = jnp.where(even_l, high, low)
        odd_ref[g] = jnp.where(even_l, low, high)


def lane_pack_kernel(chain, u_hbm, f_hbm, m_hbm, got_e, got_o, even_ref, odd_ref, tiles, sems):
    even_b, low_b, high_b = place("band")
    even_l, _, _ = place("lane")
    rows, columns = u_hbm.shape[0], u_hbm.shape[1]
    layers = pl.ds(chain * LANES, LANES)
    copies = []
    for side, start in enumerate((0, columns - TILE)):
        for part, hbm in enumerate((u_hbm, f_hbm, m_hbm)):
            copy = pltpu.make_async_copy(
                hbm.at[:, pl.ds(start, TILE), layers],
                tiles.at[3 * side + part],
                sems.at[3 * side + part],
            )
            copy.start()
            copies.append(copy)

    def message(side):
        at = pl.ds(side * (columns - TILE), TILE)
        low_rows, high_rows = by_side(even_b, got_e[:10, at, :], got_o[:10, at, :])
        zero = jnp.zeros((1, TILE, LANES), jnp.float32)
        own = [tiles[3 * side + part] for part in range(3)]
        u = jnp.concatenate([low_rows[:4], own[0], high_rows[:4]], axis=0)
        f = jnp.concatenate([zero, low_rows[4:7], own[1], high_rows[4:7], zero], axis=0)
        m = jnp.concatenate([zero, low_rows[7:10], own[2], high_rows[7:10], zero], axis=0)
        w = 0.8 / (4.0 + m)
        w = jnp.concatenate(
            [
                jnp.where(low_b, w[:4], 0.0),
                w[4 : 4 + rows],
                jnp.where(high_b, w[4 + rows :], 0.0),
            ],
            axis=0,
        )
        up = jnp.concatenate([zero, u[:-1]], axis=0)
        down = jnp.concatenate([u[1:], zero], axis=0)
        v = new_value(u, roll(u, 1, 1), roll(u, -1, 1), up, down, f, w)
        s = sublane(u)
        if side:
            f_m = jnp.where(s >= 2, roll(f, -4, 1), roll(m, -6, 1))
            return jnp.where(s >= 6, u, jnp.where(s >= 4, roll(v, -1, 1), f_m))
        f_m = jnp.where(s < 6, roll(f, 4, 1), roll(m, 6, 1))
        return jnp.where(s < 2, u, jnp.where(s < 4, roll(v, 1, 1), f_m))

    for copy in copies:
        copy.wait()
    low, high = message(0), message(1)
    even_ref[...] = jnp.where(even_l, high, low)
    odd_ref[...] = jnp.where(even_l, low, high)


def fine_halo(rows, columns, got_e, got_o, lane_e, lane_o, load, w):
    even_b, low_b, high_b = place("band")
    even_l, low_l, high_l = place("lane")
    own = pl.ds(TILE, columns)
    low_rows, high_rows = by_side(even_b, got_e[4:10], got_o[4:10])
    load[1:4, own, :] = low_rows[:3]
    w[1:4, own, :] = weight(low_rows[3:], low_b)
    load[pl.ds(FINE + rows, 3), own, :] = high_rows[:3]
    w[pl.ds(FINE + rows, 3), own, :] = weight(high_rows[3:], high_b)

    def lane_row(r, _):
        low, high = by_side(even_l, lane_e[r], lane_o[r])
        s = sublane(low)
        inside_row = ((r >= FINE) | low_b) & ((r < FINE + rows) | high_b)
        load[r, pl.ds(0, TILE), :] = roll(low, 4, 0)
        load[r, pl.ds(TILE + columns, TILE), :] = roll(high, -4, 0)
        w[r, pl.ds(0, TILE), :] = weight(roll(low, 6, 0), (s >= 6) & inside_row & low_l)
        w[r, pl.ds(TILE + columns, TILE), :] = weight(
            roll(high, -6, 0), (s < 2) & inside_row & high_l
        )
        return 0

    lax.fori_loop(0, rows + 2 * FINE, lane_row, 0, unroll=4)


def own_weight(m_own, w):
    rows, columns = m_own.shape[0], m_own.shape[1]

    def row(r, _):
        w[FINE + r, pl.ds(TILE, columns), :] = 0.8 / (4.0 + m_own[r])
        return 0

    lax.fori_loop(0, rows, row, 0, unroll=2)


def sweep(source, target, load, w, first, last):
    def row(r, carry):
        up, here = carry
        down = source[r + 1]
        target[r] = new_value(here, roll(here, 1, 0), roll(here, -1, 0), up, down, load[r], w[r])
        return here, down

    lax.fori_loop(first, last, row, (source[first - 1], source[first]), unroll=2)


def before_kernel(
    chain, u_hbm, f_hbm, m_hbm, got_e, got_o, lane_e, lane_o,
    v_ref, load_ref, even_ref, odd_ref, a, b, load, w, m_own, pairs, sems,
):
    even_b, even_l = place("band")[0], place("lane")[0]
    rows, columns = m_own.shape[0], m_own.shape[1]
    half_columns = columns // 2
    inner, own = pl.ds(FINE, rows), pl.ds(TILE, columns)
    left, right = pl.ds(0, TILE), pl.ds(TILE + columns, TILE)
    layers = pl.ds(chain * LANES, LANES)
    copies = [
        pltpu.make_async_copy(m_hbm.at[:, :, layers], m_own, sems.at[0]),
        pltpu.make_async_copy(f_hbm.at[:, :, layers], load.at[inner, own, :], sems.at[1]),
        pltpu.make_async_copy(u_hbm.at[:, :, layers], a.at[inner, own, :], sems.at[2]),
    ]
    for copy in copies:
        copy.start()
    fine_halo(rows, columns, got_e, got_o, lane_e, lane_o, load, w)
    low_rows, high_rows = by_side(even_b, got_e[:4], got_o[:4])
    a[:4, own, :] = low_rows
    a[pl.ds(FINE + rows, 4), own, :] = high_rows

    def lane_row(r, _):
        low, high = by_side(even_l, lane_e[r], lane_o[r])
        a[r, left, :] = low
        a[r, right, :] = high
        return 0

    end = rows + 2 * FINE
    lax.fori_loop(0, end, lane_row, 0, unroll=4)
    copies[0].wait()
    own_weight(m_own, w)
    copies[1].wait()
    copies[2].wait()
    sweep(a, b, load, w, 1, end - 1)

    def mend(r, _):
        low, high = by_side(even_l, lane_e[r], lane_o[r])
        s = sublane(low)
        b[r, left, :] = jnp.where(s == 7, b[r, left, :], roll(low, 1, 0))
        b[r, right, :] = jnp.where(s == 0, b[r, right, :], roll(high, -1, 0))
        return 0

    lax.fori_loop(1, end - 1, mend, 0, unroll=2)
    sweep(b, a, load, w, 2, end - 2)
    sweep(a, b, load, w, 3, end - 3)

    def defect_of(i, up, here, down):
        around = (up + down) + (roll(here, 1, 0) + roll(here, -1, 0))
        value = lax.slice_in_dim(load[FINE + i] + around, TILE, TILE + columns, axis=0)
        mine = lax.slice_in_dim(here, TILE, TILE + columns, axis=0)
        return value - (4.0 + m_own[i]) * mine

    even_columns, odd_columns = pl.ds(0, half_columns, 2), pl.ds(1, half_columns, 2)

    def restrict(k, carry):
        up, here = carry
        i = 2 * k
        middle, down = b[FINE + i + 1], b[FINE + i + 2]
        first = defect_of(i, up, here, middle)
        second = defect_of(i + 1, here, middle, down)
        v_ref[FINE + i] = here
        v_ref[FINE + i + 1] = middle
        pairs[k] = first + second
        load_ref[k] = 0.5 * (pairs[k, even_columns, :] + pairs[k, odd_columns, :])
        return middle, down

    lax.fori_loop(0, rows // 2, restrict, (b[FINE - 1], b[FINE]))
    v_ref[FINE - 1] = b[FINE - 1]
    v_ref[FINE + rows] = b[FINE + rows]
    for side, target in enumerate((even_ref, odd_ref)):
        start = edges(even_b, rows // 2, DEEP)[side]
        target[:DEEP] = load_ref[pl.ds(start, DEEP)]
        start = FINE + (jnp.where(even_b, rows - 3, 1) if side == 0 else jnp.where(even_b, 1, rows - 3))
        for k in range(4):
            at = pl.ds(TILE + k % 2 * half_columns, half_columns)
            target[DEEP + k] = v_ref[start + k // 2, at, :]


def coarse_pack_kernel(chain, load_ref, v_ref, got_e, got_o, even_ref, odd_ref):
    even_b, even_l = place("band")[0], place("lane")[0]
    half = load_ref.shape[1]
    rows, columns = v_ref.shape[0] - 2 * FINE, v_ref.shape[1] - 2 * TILE
    zero = jnp.zeros((1, TILE, LANES), jnp.float32)

    def message(side):
        at = pl.ds(side * (half - TILE), TILE)
        low, top = by_side(even_b, got_e[:, at, :], got_o[:, at, :])
        load = fold(jnp.concatenate([low[:DEEP], load_ref[:, at, :], top[:DEEP]], axis=0), side)
        near = -1 if side else 1
        tile = pl.ds(TILE + side * (columns - TILE), TILE)
        v = v_ref[pl.ds(FINE - 1, rows + 2), tile, :]
        below = roll(low[DEEP + 2 + side][None], near, 1)
        above = roll(top[DEEP + side][None], near, 1)
        v = jnp.concatenate([zero, zero, below, v, above, zero, zero], axis=0)
        quarter = v.shape[0] // 4
        first = 5 if side else 1
        parts = [roll(v[g * quarter : (g + 1) * quarter], 2 * g - first, 1) for g in range(4)]
        s = sublane(parts[0])
        v = jnp.where(
            s < 4, jnp.where(s < 2, parts[0], parts[1]), jnp.where(s < 6, parts[2], parts[3])
        )
        return jnp.concatenate([load, v], axis=0)

    low, high = message(0), message(1)
    even_ref[...] = jnp.where(even_l, high, low)
    odd_ref[...] = jnp.where(even_l, low, high)


def coarse_fields(
    group, load_ref, mass_ref, load_e, load_o, mass_e, mass_o, load_lane_e, load_lane_o, mass_lane_e, mass_lane_o, load, w
):
    even_b, low_b, high_b = place("band")
    even_l, low_l, high_l = place("lane")
    rows, columns = load_ref.shape[0], load_ref.shape[1]
    own = pl.ds(TILE, columns)

    def copy_row(r, _):
        load[DEEP + r, own, :] = load_ref[r]
        w[DEEP + r, own, :] = 0.8 / (4.0 + mass_ref[group, r])
        return 0

    lax.fori_loop(0, rows, copy_row, 0, unroll=4)
    low, high = by_side(even_b, load_e[:DEEP], load_o[:DEEP])
    load[:DEEP, own, :] = low
    load[pl.ds(DEEP + rows, DEEP), own, :] = high
    low, high = by_side(even_b, mass_e[group], mass_o[group])
    w[:DEEP, own, :] = weight(low, low_b)
    w[pl.ds(DEEP + rows, DEEP), own, :] = weight(high, high_b)
    left, right = pl.ds(0, TILE), pl.ds(TILE + columns, TILE)

    def put_load(r, low, high):
        load[r, left, :] = low
        load[r, right, :] = high

    def put_weight(r, low, high):
        inside_row = ((r >= DEEP) | low_b) & ((r < DEEP + rows) | high_b)
        w[r, left, :] = weight(low, inside_row & low_l)
        w[r, right, :] = weight(high, inside_row & high_l)

    unfold(lambda k: load_lane_e[k], lambda k: load_lane_o[k], even_l, rows, put_load)
    unfold(lambda k: mass_lane_e[group, k], lambda k: mass_lane_o[group, k], even_l, rows, put_weight)
    zero = jnp.zeros((TILE, LANES), jnp.float32)
    for r in (0, rows + 2 * DEEP - 1):
        put_load(r, zero, zero)
        w[r, left, :] = zero
        w[r, right, :] = zero


def coarse_kernel(chain, *refs):
    fields, (x_ref, even_ref, odd_ref, a, b, load, w) = refs[:10], refs[10:]
    rows, columns = x_ref.shape[0], x_ref.shape[1]
    coarse_fields(chain, *fields, load, w)
    total = rows + 2 * DEEP

    def first(r, _):
        a[r] = w[r] * load[r]
        return 0

    lax.fori_loop(0, total, first, 0, unroll=4)
    source, target = a, b
    for step in range(1, FIRST_SWEEPS):
        sweep(source, target, load, w, step, total - step)
        source, target = target, source

    def out(r, _):
        x_ref[r] = source[DEEP + r, pl.ds(TILE, columns), :]
        return 0

    lax.fori_loop(0, rows, out, 0, unroll=4)
    for side, target in enumerate((even_ref, odd_ref)):
        start = edges(place("band")[0], rows, SECOND)[side]
        target[...] = x_ref[pl.ds(start, SECOND)]


def value_pack_kernel(chain, x_ref, got_e, got_o, even_ref, odd_ref):
    even_b, even_l = place("band")[0], place("lane")[0]
    zero = jnp.zeros((DEEP - SECOND, TILE, LANES), jnp.float32)

    def message(side):
        at = pl.ds(side * (x_ref.shape[1] - TILE), TILE)
        low, high = by_side(even_b, got_e[:, at, :], got_o[:, at, :])
        return fold(jnp.concatenate([zero, low, x_ref[:, at, :], high, zero], axis=0), side)

    low, high = message(0), message(1)
    even_ref[...] = jnp.where(even_l, high, low)
    odd_ref[...] = jnp.where(even_l, low, high)


def after_kernel(
    chain, f_hbm, m_hbm, v_ref, x_ref, fine_e, fine_o, fine_lane_e, fine_lane_o, *refs
):
    fields, (value_e, value_o, value_lane_e, value_lane_o), rest = refs[:10], refs[10:14], refs[14:]
    u_hbm, d_hbm, a, b, load, w, m_own, x, y, coarse_load, coarse_w, spread, sems = rest[-13:]
    _, _, coarse_e, coarse_o, _, _, coarse_lane_e, coarse_lane_o, _, _ = fields
    even_b, even_l = place("band")[0], place("lane")[0]
    rows, columns = m_own.shape[0], m_own.shape[1]
    half_rows, half_columns = rows // 2, columns // 2
    layers = pl.ds(chain * LANES, LANES)
    inner, fine_own = pl.ds(FINE, rows), pl.ds(TILE, columns)
    left, right = pl.ds(0, TILE), pl.ds(TILE + columns, TILE)
    copies = [
        pltpu.make_async_copy(m_hbm.at[:, :, layers], m_own, sems.at[0]),
        pltpu.make_async_copy(f_hbm.at[:, :, layers], load.at[inner, fine_own, :], sems.at[1]),
    ]
    for copy in copies:
        copy.start()
    coarse_fields(chain, *fields, coarse_load, coarse_w)
    own = pl.ds(TILE, half_columns)
    total = half_rows + 2 * DEEP
    low, high = by_side(even_b, value_e[...], value_o[...])
    x[DEEP - SECOND : DEEP, own, :] = low
    x[pl.ds(DEEP + half_rows, SECOND), own, :] = high

    def coarse_copy(r, _):
        x[DEEP + r, own, :] = x_ref[r]
        return 0

    lax.fori_loop(0, half_rows, coarse_copy, 0, unroll=4)

    def put_value(r, low, high):
        x[r, pl.ds(0, TILE), :] = low
        x[r, pl.ds(TILE + half_columns, TILE), :] = high

    unfold(lambda k: value_lane_e[k], lambda k: value_lane_o[k], even_l, half_rows, put_value)
    source, target = x, y
    for step in range(1, LAST_SWEEPS + 1):
        edge = DEEP - SECOND + step
        sweep(source, target, coarse_load, coarse_w, edge, total - edge)
        source, target = target, source

    fine_halo(rows, columns, fine_e, fine_o, fine_lane_e, fine_lane_o, load, w)
    copies[0].wait()
    own_weight(m_own, w)

    a[FINE - 1] = v_ref[FINE - 1]
    a[FINE + rows] = v_ref[FINE + rows]
    for i in range(2):
        for part in range(2):
            at = pl.ds(TILE + part * half_columns, half_columns)
            k = DEEP + 2 * i + part
            low, high = by_side(even_b, coarse_e[k], coarse_o[k])
            a[1 + i, at, :] = low
            a[FINE + rows + 1 + i, at, :] = high
    end = rows + 2 * FINE
    quarter = end // 4
    above = DEEP - 1 + half_rows

    def fine_lane(k, _):
        low, high = by_side(even_l, coarse_lane_e[above + k], coarse_lane_o[above + k])
        s = sublane(low)
        for g in range(4):
            r = g * quarter + k
            second = (r == FINE - 2) | (r == FINE + rows + 1)
            deep_low, deep_high = roll(low, 5 - 2 * g, 0), roll(high, 1 - 2 * g, 0)
            near_low = jnp.where(second, roll(deep_low, 1, 0), v_ref[r, left, :])
            near_high = jnp.where(second, roll(deep_high, -1, 0), v_ref[r, right, :])
            a[r, left, :] = jnp.where(s == TILE - 1, near_low, deep_low)
            a[r, right, :] = jnp.where(s == 0, near_high, deep_high)
        return 0

    lax.fori_loop(0, quarter, fine_lane, 0, unroll=2)
    across = columns // 2 + TILE
    skip = TILE - TILE // 2

    def spread_row(k):
        value = source[DEEP - 2 + k, pl.ds(skip, across), :]
        spread[k, pl.ds(0, across, 2), :] = value
        spread[k, pl.ds(1, across, 2), :] = value
        return spread[k]

    for k in (0, 1, half_rows + 2, half_rows + 3):
        both = spread_row(k)
        a[2 * k] += both
        a[2 * k + 1] += both

    def correct(k, _):
        both = spread_row(k)
        ends = [lax.slice_in_dim(both, s, s + TILE, axis=0) for s in (0, TILE + columns)]
        middle = lax.slice_in_dim(both, TILE, TILE + columns, axis=0)
        for part in range(2):
            r = 2 * k + part
            a[r, fine_own, :] = v_ref[r, fine_own, :] + middle
            a[r, left, :] += ends[0]
            a[r, right, :] += ends[1]
        return 0

    lax.fori_loop(2, half_rows + 2, correct, 0, unroll=2)
    copies[1].wait()
    sweep(a, b, load, w, 2, end - 2)
    sweep(b, a, load, w, 3, end - 3)
    piece = rows // CHUNKS

    def put(source, hbm, at, sem):
        copy = pltpu.make_async_copy(
            source.at[pl.ds(FINE + at, piece), fine_own, :],
            hbm.at[pl.ds(at, piece), :, layers],
            sem,
        )
        copy.start()
        return copy

    puts = [put(a, u_hbm, c * piece, sems.at[2 + c]) for c in range(CHUNKS)]

    def remains(i, carry):
        up, here = carry
        down = a[FINE + i + 1]
        around = (up + down) + (roll(here, 1, 0) + roll(here, -1, 0))
        value = lax.slice_in_dim(load[FINE + i] + around, TILE, TILE + columns, axis=0)
        mine = lax.slice_in_dim(here, TILE, TILE + columns, axis=0)
        b[FINE + i, fine_own, :] = value - (4.0 + m_own[i]) * mine
        return here, down

    carry = (a[FINE - 1], a[FINE])
    for c in range(CHUNKS):
        carry = lax.fori_loop(c * piece, (c + 1) * piece, remains, carry, unroll=2)
        puts.append(put(b, d_hbm, c * piece, sems.at[2 + CHUNKS + c]))
    for copy in puts:
        copy.wait()


def call(kernel, chain, outs, args, limit, scratch=(), sems=0, hbm=0, hbm_out=False, aliases=None, extra=0, us=1):
    far, near = pl.BlockSpec(memory_space=pltpu.HBM), pl.BlockSpec(memory_space=pltpu.VMEM)
    near_count = len(args) - hbm - extra
    return pl.pallas_call(
        functools.partial(kernel, chain),
        in_specs=[far] * hbm + [near] * near_count + [far] * extra,
        out_specs=[far if hbm_out else near] * len(outs),
        out_shape=[jax.ShapeDtypeStruct(s, jnp.float32) for s in outs],
        scratch_shapes=[pltpu.VMEM(s + (LANES,), jnp.float32) for s in scratch]
        + ([pltpu.SemaphoreType.DMA((sems,))] if sems else []),
        input_output_aliases=aliases or {},
        cost_estimate=pl.CostEstimate(flops=us * COST, bytes_accessed=0, transcendentals=0),
        compiler_params=pltpu.CompilerParams(vmem_limit_bytes=limit * 1024 * 1024),
    )(*args)


def program(f, u, m):
    rows, columns, layers = f.shape
    half_rows, half_columns = rows // 2, columns // 2
    end, total = rows + 2 * FINE, half_rows + 2 * DEEP
    folded = DEEP - 1 + half_rows
    wide, half_wide = columns + 2 * TILE, half_columns + 2 * TILE
    groups = layers // LANES
    coarse_block = (half_rows, half_columns, LANES)
    chains = range(groups)

    fines = []
    for c in chains:
        even, odd = call(first_kernel, c, [(10, columns, LANES)] * 2, (u, f, m), FAR, sems=6, hbm=3)
        fines.append(swap("band", even, odd))
    mass, even, odd = call(
        mass_kernel, 0, [(groups,) + coarse_block] + [(groups, DEEP, half_columns, LANES)] * 2, (m,), MASS,
        scratch=[(groups, rows, columns), (half_rows, columns)], sems=groups, hbm=1,
    )
    masses = swap("band", even, odd)
    fine_lanes = []
    for c in chains:
        even, odd = call(
            lane_pack_kernel, c, [(end, TILE, LANES)] * 2, (u, f, m, *fines[c]), NEAR,
            scratch=[(6, rows, TILE)], sems=6, hbm=3,
        )
        fine_lanes.append(swap("lane", even, odd))
    even, odd = call(mass_pack_kernel, 0, [(groups, folded, TILE, LANES)] * 2, (mass, *masses), 4)
    mass_lanes = swap("lane", even, odd)
    values, loads, coarses = [], [], []
    for c in chains:
        v, load, even, odd = call(
            before_kernel, c, [(end, wide, LANES), coarse_block] + [(DEEP + 4, half_columns, LANES)] * 2,
            (u, f, m, *fines[c], *fine_lanes[c]), BEFORE, us=6,
            scratch=[(end, wide)] * 4 + [(rows, columns), (half_rows, columns)], sems=3, hbm=3,
        )
        values.append(v)
        loads.append(load)
        coarses.append(swap("band", even, odd))
    coarse_lanes = []
    for c in chains:
        even, odd = call(
            coarse_pack_kernel, c, [(folded + end // 4, TILE, LANES)] * 2, (loads[c], values[c], *coarses[c]), 4,
        )
        coarse_lanes.append(swap("lane", even, odd))
    fields, xs, nexts = [], [], []
    for c in chains:
        fields.append((loads[c], mass, *coarses[c], *masses, *coarse_lanes[c], *mass_lanes))
        x, even, odd = call(
            coarse_kernel, c, [coarse_block] + [(SECOND, half_columns, LANES)] * 2, fields[c], 8, us=4,
            scratch=[(total, half_wide)] * 4,
        )
        xs.append(x)
        nexts.append(swap("band", even, odd))
    next_lanes = []
    for c in chains:
        even, odd = call(value_pack_kernel, c, [(folded, TILE, LANES)] * 2, (xs[c], *nexts[c]), 4)
        next_lanes.append(swap("lane", even, odd))
    results = ()
    for c in chains:
        args = (f, m, values[c], xs[c], *fines[c], *fine_lanes[c], *fields[c], *nexts[c], *next_lanes[c])
        results = tuple(
            call(
                after_kernel, c, [(rows, columns, layers)] * 2, args + results, AFTER, us=8,
                scratch=[(end, wide)] * 4 + [(rows, columns)] + [(total, half_wide)] * 4 + [(half_rows + 4, wide)],
                sems=2 + 2 * CHUNKS, hbm=2, hbm_out=True, extra=len(results),
                aliases={len(args) + k: k for k in range(len(results))},
            )
        )
    return results


def solution(mesh):
    return jax.shard_map(
        program,
        mesh=mesh,
        in_specs=(P("band", "lane", None), P("band", "lane", None), P("band", "lane", None)),
        out_specs=(P("band", "lane", None), P("band", "lane", None)),
        check_vma=False,
    )
```

```python
import functools

import jax
import jax.numpy as jnp
from jax import lax
from jax.experimental import pallas as pl
from jax.experimental.pallas import tpu as pltpu
from jax.sharding import PartitionSpec as P


LANES = 128
INNER = 13
FINE = 4
TILE = 8
DEEP = 8
SECOND = 6
FIRST_SWEEPS = DEEP + 1
LAST_SWEEPS = INNER - FIRST_SWEEPS
CHUNKS = 4
FAR = 60
LOAD = 39
COST = 500_000_000


def swaps(count, first):
    pairs = []
    for i in range(first, count - 1, 2):
        pairs += [(i, i + 1), (i + 1, i)]
    return pairs


def swap(axis, even, odd):
    count = lax.axis_size(axis)
    return (
        lax.ppermute(even, axis, swaps(count, 0)),
        lax.ppermute(odd, axis, swaps(count, 1)),
    )


def place(axis):
    at, count = lax.axis_index(axis), lax.axis_size(axis)
    return lax.rem(at, 2) == 0, at > 0, at < count - 1


def roll(value, shift, axis):
    return pltpu.roll(value, shift % value.shape[axis], axis)


def sublane(value):
    return lax.broadcasted_iota(jnp.int32, value.shape, value.ndim - 2)


def by_side(even, got_even, got_odd):
    low = jnp.where(even, got_odd, got_even)
    high = jnp.where(even, got_even, got_odd)
    return low, high


def weight(mass, inside):
    return jnp.where(inside, 0.8 / (4.0 + mass), 0.0)


def new_value(here, left, right, up, down, load, w):
    return 0.2 * here + w * (load + ((up + down) + (left + right)))


def edges(even, rows, depth):
    return jnp.where(even, rows - depth, 0), jnp.where(even, 0, rows - depth)


def packed(u, f, m, v, side):
    s = sublane(u)
    if side:
        f_m = jnp.where(s >= 2, roll(f, -4, 1), roll(m, -6, 1))
        return jnp.where(s >= 6, u, jnp.where(s >= 4, roll(v, -1, 1), f_m))
    f_m = jnp.where(s < 6, roll(f, 4, 1), roll(m, 6, 1))
    return jnp.where(s < 2, u, jnp.where(s < 4, roll(v, 1, 1), f_m))


def swept(u, f, w):
    zero = jnp.zeros((1,) + u.shape[1:], jnp.float32)
    up = jnp.concatenate([zero, u[:-1]], axis=0)
    down = jnp.concatenate([u[1:], zero], axis=0)
    return new_value(u, roll(u, 1, 1), roll(u, -1, 1), up, down, f, w)


def put_sides(even, make, even_ref, odd_ref):
    low, high = make(0), make(1)
    even_ref[...] = jnp.where(even, high, low)
    odd_ref[...] = jnp.where(even, low, high)


def first_kernel(chain, u_hbm, f_hbm, m_hbm, *refs):
    even_b, even_l = place("band")[0], place("lane")[0]
    rows, columns, _ = m_hbm.shape
    arrays = (u_hbm, f_hbm, m_hbm)
    outs, (tiles, sems) = refs[:-2], refs[-2:]
    groups = len(outs) // 4
    tile_copies, copies = [], []
    for g in range(groups):
        at = pl.ds(g * LANES, LANES)
        for side in range(2):
            for part, hbm in enumerate(arrays):
                copy = pltpu.make_async_copy(
                    hbm.at[:, pl.ds(side * (columns - TILE), TILE), at],
                    tiles.at[g, 3 * side + part],
                    sems.at[12 * g + 3 * side + part],
                )
                copy.start()
                tile_copies.append(copy)
        for side, target in enumerate(outs[4 * g : 4 * g + 2]):
            for part, (hbm, depth, first) in enumerate(zip(arrays, (4, 3, 3), (0, 4, 7))):
                start = edges(even_b, rows, depth)[side]
                copy = pltpu.make_async_copy(
                    hbm.at[pl.ds(start, depth), :, at],
                    target.at[pl.ds(first, depth)],
                    sems.at[12 * g + 6 + 3 * side + part],
                )
                copy.start()
                copies.append(copy)
    for g in range(groups):
        for copy in tile_copies[6 * g : 6 * g + 6]:
            copy.wait()

        def make(side, g=g):
            u, f, m = [tiles[g, 3 * side + part] for part in range(3)]
            return packed(u, f, m, swept(u, f, 0.8 / (4.0 + m)), side)

        put_sides(even_l, make, *outs[4 * g + 2 : 4 * g + 4])
    for copy in copies:
        copy.wait()


def mass_place(group, k, half):
    return 10 + group * (DEEP // 2) + k // 2, k % 2 * half


def mass_strip(ref, group, start, width, half):
    places = [mass_place(group, k, half) for k in range(DEEP)]
    return jnp.concatenate([ref[r, pl.ds(c + start, width), :][None] for r, c in places], axis=0)


def load_kernel(chain, u_hbm, f_hbm, m_hbm, *refs):
    even_b, even_l = place("band")[0], place("lane")[0]
    owns, (mass_ref, even_ref, odd_ref, lane_e, lane_o, pairs, sems) = refs[:-7], refs[-7:]
    groups, half_rows, half = mass_ref.shape[0], mass_ref.shape[1], mass_ref.shape[2]
    rows, columns = 2 * half_rows, 2 * half
    even_columns, odd_columns = pl.ds(0, half, 2), pl.ds(1, half, 2)
    copies = [None] * len(owns)
    for g in reversed(range(groups)):
        for part, hbm in ((2, m_hbm), (1, f_hbm), (0, u_hbm)):
            k = 3 * g + part
            copies[k] = pltpu.make_async_copy(hbm.at[:, :, pl.ds(g * LANES, LANES)], owns[k], sems.at[k])
            copies[k].start()
    for g in reversed(range(groups)):
        m_ref = owns[3 * g + 2]
        copies[3 * g + 2].wait()

        def restrict(k, _, g=g, m_ref=m_ref):
            pairs[k] = m_ref[2 * k] + m_ref[2 * k + 1]
            mass_ref[g, k] = 0.5 * (pairs[k, even_columns, :] + pairs[k, odd_columns, :])
            return 0

        lax.fori_loop(0, half_rows, restrict, 0, unroll=2)
        for side, target in enumerate((even_ref, odd_ref)):
            start = edges(even_b, half_rows, DEEP)[side]
            for k in range(DEEP):
                r, c = mass_place(g, k, half)
                target[r, pl.ds(c, half), :] = mass_ref[g, start + k]
    own = owns[3 * groups - 3 :]
    for copy in copies[3 * groups - 3 : 3 * groups - 1]:
        copy.wait()
    for side, target in enumerate((even_ref, odd_ref)):
        for ref, depth, at in zip(own, (4, 3, 3), (0, 4, 7)):
            target[pl.ds(at, depth)] = ref[pl.ds(edges(even_b, rows, depth)[side], depth)]

    def make(side):
        at = pl.ds(side * (columns - TILE), TILE)
        u, f, m = [ref[:, at, :] for ref in own]
        at = pl.ds(side * (half - TILE), TILE)
        parts = [packed(u, f, m, swept(u, f, 0.8 / (4.0 + m)), side)]
        return jnp.concatenate(parts + [mass_ref[g, :, at, :] for g in range(groups)], axis=0)

    put_sides(even_l, make, lane_e, lane_o)
    for g in range(groups - 1):
        for copy in copies[3 * g : 3 * g + 2]:
            copy.wait()


def fold(low, high, side):
    depth = DEEP
    s = sublane(low[0])
    merged = []
    for r in range(1, depth):
        if side:
            merged.append(jnp.where(s >= depth - r, low[r], roll(high[r - 1], -r, 0))[None])
        else:
            merged.append(jnp.where(s < r, low[r], roll(high[r - 1], r, 0))[None])
    return jnp.concatenate(merged, axis=0)


def unfold(got_e, got_o, corner_e, corner_o, even, rows, write):
    def own(k, _):
        low, high = by_side(even, got_e(k), got_o(k))
        write(DEEP + k, low, high)
        return 0

    lax.fori_loop(0, rows, own, 0, unroll=4)
    for r in range(1, DEEP):
        low, high = by_side(even, corner_e(r - 1), corner_o(r - 1))
        write(r, low, high)
        write(DEEP + rows - 1 + r, roll(low, r, 0), roll(high, -r, 0))


CORNER = FINE + 1


def fine_corner_kernel(chain, u_ref, f_ref, m_ref, got_e, got_o, *refs):
    even_ref, odd_ref = refs[-2:]
    even_b, low_b, high_b = place("band")
    rows, columns = u_ref.shape[0], u_ref.shape[1]
    zero = jnp.zeros((1, TILE, LANES), jnp.float32)

    def make(side):
        at = pl.ds(side * (columns - TILE), TILE)
        low, high = by_side(even_b, got_e[:, at, :], got_o[:, at, :])
        parts = []
        for top, inside, halo in ((True, low_b, low), (False, high_b, high)):
            near = pl.ds(0 if top else rows - 2, 2)
            own = [ref[near, at, :] for ref in (u_ref, f_ref, m_ref)]
            h = [halo[:4], halo[4:7], halo[7:10]]
            if top:
                u, f, m = (
                    jnp.concatenate([h[0], own[0]], axis=0),
                    jnp.concatenate([zero, h[1], own[1]], axis=0),
                    jnp.concatenate([zero, h[2], own[2]], axis=0),
                )
            else:
                u, f, m = (
                    jnp.concatenate([own[0], h[0]], axis=0),
                    jnp.concatenate([own[1], h[1], zero], axis=0),
                    jnp.concatenate([own[2], h[2], zero], axis=0),
                )
            w = 0.8 / (4.0 + m)
            if top:
                w = jnp.concatenate([jnp.where(inside, w[:4], 0.0), w[4:]], axis=0)
            else:
                w = jnp.concatenate([w[:2], jnp.where(inside, w[2:], 0.0)], axis=0)
            message = packed(u, f, m, swept(u, f, w), side)
            parts.append(message[:CORNER] if top else message[1:])
        return jnp.concatenate(parts, axis=0)

    put_sides(place("lane")[0], make, even_ref, odd_ref)


def fine_lane_rows(rows, lanes, even, write):
    lane_e, lane_o, corner_e, corner_o = lanes

    def own(r, _):
        low, high = by_side(even, lane_e[r - FINE], lane_o[r - FINE])
        write(r, low, high)
        return 0

    for k in range(CORNER):
        for r, at in ((k, k), (rows + FINE - 1 + k, CORNER + k)):
            low, high = by_side(even, corner_e[at], corner_o[at])
            write(r, low, high)
    lax.fori_loop(CORNER, rows + FINE - 1, own, 0, unroll=2)


def fine_halo(rows, columns, got_e, got_o, lanes, load, w):
    even_b, low_b, high_b = place("band")
    even_l, low_l, high_l = place("lane")
    own = pl.ds(TILE, columns)
    low_rows, high_rows = by_side(even_b, got_e[4:10], got_o[4:10])
    load[1:4, own, :] = low_rows[:3]
    w[1:4, own, :] = weight(low_rows[3:], low_b)
    load[pl.ds(FINE + rows, 3), own, :] = high_rows[:3]
    w[pl.ds(FINE + rows, 3), own, :] = weight(high_rows[3:], high_b)

    def write(r, low, high):
        s = sublane(low)
        inside_row = ((r >= FINE) | low_b) & ((r < FINE + rows) | high_b)
        load[r, pl.ds(0, TILE), :] = roll(low, 4, 0)
        load[r, pl.ds(TILE + columns, TILE), :] = roll(high, -4, 0)
        w[r, pl.ds(0, TILE), :] = weight(roll(low, 6, 0), (s >= 6) & inside_row & low_l)
        w[r, pl.ds(TILE + columns, TILE), :] = weight(
            roll(high, -6, 0), (s < 2) & inside_row & high_l
        )

    fine_lane_rows(rows, lanes, even_l, write)


def own_fields(f_ref, m_ref, load, w):
    rows, columns = m_ref.shape[0], m_ref.shape[1]
    own = pl.ds(TILE, columns)

    def row(r, _):
        load[FINE + r, own, :] = f_ref[r]
        w[FINE + r, own, :] = 0.8 / (4.0 + m_ref[r])
        return 0

    lax.fori_loop(0, rows, row, 0, unroll=2)


def sweep(source, target, load, w, first, last):
    def row(r, carry):
        up, here = carry
        down = source[r + 1]
        target[r] = new_value(here, roll(here, 1, 0), roll(here, -1, 0), up, down, load[r], w[r])
        return here, down

    lax.fori_loop(first, last, row, (source[first - 1], source[first]), unroll=2)


def before_kernel(
    chain, u_ref, f_ref, m_own, got_e, got_o, lane_e, lane_o, corner_e, corner_o,
    v_ref, load_ref, even_ref, odd_ref, a, b, load, w, pairs,
):
    even_b, even_l = place("band")[0], place("lane")[0]
    rows, columns = m_own.shape[0], m_own.shape[1]
    half_columns = columns // 2
    own = pl.ds(TILE, columns)
    left, right = pl.ds(0, TILE), pl.ds(TILE + columns, TILE)
    lanes = (lane_e, lane_o, corner_e, corner_o)
    own_fields(f_ref, m_own, load, w)
    fine_halo(rows, columns, got_e, got_o, lanes, load, w)
    low_rows, high_rows = by_side(even_b, got_e[:4], got_o[:4])
    a[:4, own, :] = low_rows
    a[pl.ds(FINE + rows, 4), own, :] = high_rows

    def copy_row(r, _):
        a[FINE + r, own, :] = u_ref[r]
        return 0

    lax.fori_loop(0, rows, copy_row, 0, unroll=2)

    def put_lane(r, low, high):
        a[r, left, :] = low
        a[r, right, :] = high

    fine_lane_rows(rows, lanes, even_l, put_lane)
    end = rows + 2 * FINE
    sweep(a, b, load, w, 1, end - 1)

    def mend(r, low, high):
        s = sublane(low)
        b[r, left, :] = jnp.where(s == 7, b[r, left, :], roll(low, 1, 0))
        b[r, right, :] = jnp.where(s == 0, b[r, right, :], roll(high, -1, 0))

    fine_lane_rows(rows, lanes, even_l, mend)
    sweep(b, a, load, w, 2, end - 2)
    sweep(a, b, load, w, 3, end - 3)

    def defect_of(i, up, here, down):
        around = (up + down) + (roll(here, 1, 0) + roll(here, -1, 0))
        value = lax.slice_in_dim(load[FINE + i] + around, TILE, TILE + columns, axis=0)
        mine = lax.slice_in_dim(here, TILE, TILE + columns, axis=0)
        return value - (4.0 + m_own[i]) * mine

    even_columns, odd_columns = pl.ds(0, half_columns, 2), pl.ds(1, half_columns, 2)

    def restrict(k, carry):
        up, here = carry
        i = 2 * k
        middle, down = b[FINE + i + 1], b[FINE + i + 2]
        first = defect_of(i, up, here, middle)
        second = defect_of(i + 1, here, middle, down)
        v_ref[FINE + i] = here
        v_ref[FINE + i + 1] = middle
        pairs[k] = first + second
        load_ref[k] = 0.5 * (pairs[k, even_columns, :] + pairs[k, odd_columns, :])
        return middle, down

    lax.fori_loop(0, rows // 2, restrict, (b[FINE - 1], b[FINE]))
    v_ref[FINE - 1] = b[FINE - 1]
    v_ref[FINE + rows] = b[FINE + rows]
    for r in range(FINE - 1):
        v_ref[r] = jnp.zeros_like(b[0])
        v_ref[end - 1 - r] = jnp.zeros_like(b[0])
    for side, target in enumerate((even_ref, odd_ref)):
        start = edges(even_b, rows // 2, DEEP)[side]
        target[:DEEP] = load_ref[pl.ds(start, DEEP)]
        start = FINE + (jnp.where(even_b, rows - 3, 1) if side == 0 else jnp.where(even_b, 1, rows - 3))
        for k in range(4):
            at = pl.ds(TILE + k % 2 * half_columns, half_columns)
            target[DEEP + k] = v_ref[start + k // 2, at, :]


def coarse_pack_kernel(chain, load_ref, v_ref, got_e, got_o, mass_e, mass_o, *refs):
    even_ref, odd_ref = refs[-2:]
    even_b, even_l = place("band")[0], place("lane")[0]
    half, columns = got_e.shape[1], v_ref.shape[1] - 2 * TILE

    def make(side):
        at = pl.ds(side * (half - TILE), TILE)
        tile = pl.ds(TILE + side * (columns - TILE), TILE)
        quarter, first = v_ref.shape[0] // 4, 5 if side else 1
        turned = [
            roll(v_ref[pl.ds(g * quarter, quarter), tile, :], 2 * g - first, 1) for g in range(4)
        ]
        s = sublane(turned[0])
        v = jnp.where(
            s < 4, jnp.where(s < 2, turned[0], turned[1]), jnp.where(s < 6, turned[2], turned[3])
        )
        low, high = by_side(even_b, got_e[:, at, :], got_o[:, at, :])
        load = fold(low[:DEEP], high[:DEEP], side)
        below, above = low[DEEP + 2 + side], high[DEEP + side]
        s = sublane(below)
        keep = s >= 4 if side else s < 4
        second = jnp.where(keep, below, roll(above, 4, 0))[None]
        start = side * (half - TILE)
        low, high = by_side(
            even_b, *[mass_strip(ref, chain, start, TILE, half) for ref in (mass_e, mass_o)]
        )
        return jnp.concatenate([load_ref[:, at, :], v, load, fold(low, high, side), second], axis=0)

    put_sides(even_l, make, even_ref, odd_ref)


def coarse_fields(
    group, load_ref, mass_ref, load_e, load_o, mass_e, mass_o, load_lane_e, load_lane_o, mass_lane_e, mass_lane_o, load, w
):
    even_b, low_b, high_b = place("band")
    even_l, low_l, high_l = place("lane")
    rows, columns = load_ref.shape[0], load_ref.shape[1]
    own = pl.ds(TILE, columns)

    def copy_row(r, _):
        load[DEEP + r, own, :] = load_ref[r]
        w[DEEP + r, own, :] = 0.8 / (4.0 + mass_ref[group, r])
        return 0

    lax.fori_loop(0, rows, copy_row, 0, unroll=4)
    low, high = by_side(even_b, load_e[:DEEP], load_o[:DEEP])
    load[:DEEP, own, :] = low
    load[pl.ds(DEEP + rows, DEEP), own, :] = high
    low, high = by_side(
        even_b, *[mass_strip(ref, group, 0, columns, columns) for ref in (mass_e, mass_o)]
    )
    w[:DEEP, own, :] = weight(low, low_b)
    w[pl.ds(DEEP + rows, DEEP), own, :] = weight(high, high_b)
    left, right = pl.ds(0, TILE), pl.ds(TILE + columns, TILE)

    def put_load(r, low, high):
        load[r, left, :] = low
        load[r, right, :] = high

    def put_weight(r, low, high):
        inside_row = ((r >= DEEP) | low_b) & ((r < DEEP + rows) | high_b)
        w[r, left, :] = weight(low, inside_row & low_l)
        w[r, right, :] = weight(high, inside_row & high_l)

    first = load_lane_e.shape[0] - 2 * DEEP + 1
    second = first + DEEP - 1
    base = (2 + group) * rows
    unfold(
        lambda k: load_lane_e[k], lambda k: load_lane_o[k],
        lambda k: load_lane_e[first + k], lambda k: load_lane_o[first + k], even_l, rows, put_load,
    )
    unfold(
        lambda k: mass_lane_e[base + k], lambda k: mass_lane_o[base + k],
        lambda k: load_lane_e[second + k], lambda k: load_lane_o[second + k], even_l, rows, put_weight,
    )
    zero = jnp.zeros((TILE, LANES), jnp.float32)
    for r in (0, rows + 2 * DEEP - 1):
        put_load(r, zero, zero)
        w[r, left, :] = zero
        w[r, right, :] = zero


def coarse_kernel(chain, *refs):
    fields, (x_ref, even_ref, odd_ref, a, b, load, w) = refs[:10], refs[10:]
    rows, columns = x_ref.shape[0], x_ref.shape[1]
    coarse_fields(chain, *fields, load, w)
    total = rows + 2 * DEEP

    def first(r, _):
        a[r] = w[r] * load[r]
        return 0

    lax.fori_loop(0, total, first, 0, unroll=4)
    source, target = a, b
    for step in range(1, FIRST_SWEEPS):
        sweep(source, target, load, w, step, total - step)
        source, target = target, source

    def out(r, _):
        x_ref[r] = source[DEEP + r, pl.ds(TILE, columns), :]
        return 0

    lax.fori_loop(0, rows, out, 0, unroll=4)
    for side, target in enumerate((even_ref, odd_ref)):
        start = edges(place("band")[0], rows, SECOND)[side]
        target[...] = x_ref[pl.ds(start, SECOND)]


def value_pack_kernel(chain, x_ref, got_e, got_o, *refs):
    even_ref, odd_ref = refs[-2:]
    even_b, even_l = place("band")[0], place("lane")[0]
    zero = jnp.zeros((DEEP - SECOND, TILE, LANES), jnp.float32)

    def make(side):
        at = pl.ds(side * (got_e.shape[1] - TILE), TILE)
        low, high = by_side(even_b, got_e[:, at, :], got_o[:, at, :])
        low, high = jnp.concatenate([zero, low], axis=0), jnp.concatenate([high, zero], axis=0)
        return jnp.concatenate([x_ref[:, at, :], fold(low, high, side)], axis=0)

    put_sides(even_l, make, even_ref, odd_ref)


def after_kernel(
    chain, f_ref, m_own, v_ref, x_ref, fine_e, fine_o, lane_e, lane_o, corner_e, corner_o, *refs
):
    fields, (value_e, value_o, value_lane_e, value_lane_o), rest = refs[:10], refs[10:14], refs[14:]
    u_hbm, d_hbm, a, b, load, w, x, y, coarse_load, coarse_w, spread, sems = rest[-12:]
    coarse_e, coarse_o, _, _, coarse_lane_e, coarse_lane_o = fields[2:8]
    even_b, even_l = place("band")[0], place("lane")[0]
    rows, columns = m_own.shape[0], m_own.shape[1]
    half_rows, half_columns = rows // 2, columns // 2
    layers = pl.ds(chain * LANES, LANES)
    fine_own = pl.ds(TILE, columns)
    left, right = pl.ds(0, TILE), pl.ds(TILE + columns, TILE)
    coarse_fields(chain, *fields, coarse_load, coarse_w)
    own = pl.ds(TILE, half_columns)
    total = half_rows + 2 * DEEP
    low, high = by_side(even_b, value_e[...], value_o[...])
    x[DEEP - SECOND : DEEP, own, :] = low
    x[pl.ds(DEEP + half_rows, SECOND), own, :] = high

    def coarse_copy(r, _):
        x[DEEP + r, own, :] = x_ref[r]
        return 0

    lax.fori_loop(0, half_rows, coarse_copy, 0, unroll=4)

    def put_value(r, low, high):
        x[r, pl.ds(0, TILE), :] = low
        x[r, pl.ds(TILE + half_columns, TILE), :] = high

    unfold(
        lambda k: value_lane_e[k], lambda k: value_lane_o[k],
        lambda k: value_lane_e[half_rows + k], lambda k: value_lane_o[half_rows + k], even_l, half_rows, put_value,
    )
    source, target = x, y
    for step in range(1, LAST_SWEEPS + 1):
        edge = DEEP - SECOND + step
        sweep(source, target, coarse_load, coarse_w, edge, total - edge)
        source, target = target, source

    own_fields(f_ref, m_own, load, w)
    fine_halo(rows, columns, fine_e, fine_o, (lane_e, lane_o, corner_e, corner_o), load, w)

    a[FINE - 1] = v_ref[FINE - 1]
    a[FINE + rows] = v_ref[FINE + rows]
    for i in range(2):
        for part in range(2):
            at = pl.ds(TILE + part * half_columns, half_columns)
            k = DEEP + 2 * i + part
            low, high = by_side(even_b, coarse_e[k], coarse_o[k])
            a[1 + i, at, :] = low
            a[FINE + rows + 1 + i, at, :] = high
    end = rows + 2 * FINE
    quarter = end // 4
    first = half_rows

    def fine_lane(k, _):
        low, high = by_side(even_l, coarse_lane_e[first + k], coarse_lane_o[first + k])
        s = sublane(low)
        for g in range(4):
            r = g * quarter + k
            a[r, left, :] = jnp.where(s == TILE - 1, v_ref[r, left, :], roll(low, 5 - 2 * g, 0))
            a[r, right, :] = jnp.where(s == 0, v_ref[r, right, :], roll(high, 1 - 2 * g, 0))
        return 0

    lax.fori_loop(0, quarter, fine_lane, 0, unroll=2)
    at = coarse_lane_e.shape[0] - 1
    low, high = by_side(even_l, coarse_lane_e[at], coarse_lane_o[at])
    for r, turn in ((FINE - 2, 0), (FINE + rows + 1, 4)):
        a[r, left, :] = roll(low, turn, 0)
        a[r, right, :] = roll(high, turn, 0)
    across = columns // 2 + TILE
    skip = TILE - TILE // 2

    def spread_row(k):
        value = source[DEEP - 2 + k, pl.ds(skip, across), :]
        spread[k, pl.ds(0, across, 2), :] = value
        spread[k, pl.ds(1, across, 2), :] = value
        return spread[k]

    for k in (0, 1, half_rows + 2, half_rows + 3):
        both = spread_row(k)
        a[2 * k] += both
        a[2 * k + 1] += both

    def correct(k, _):
        both = spread_row(k)
        ends = [lax.slice_in_dim(both, s, s + TILE, axis=0) for s in (0, TILE + columns)]
        middle = lax.slice_in_dim(both, TILE, TILE + columns, axis=0)
        for part in range(2):
            r = 2 * k + part
            a[r, fine_own, :] = v_ref[r, fine_own, :] + middle
            a[r, left, :] += ends[0]
            a[r, right, :] += ends[1]
        return 0

    lax.fori_loop(2, half_rows + 2, correct, 0, unroll=2)
    sweep(a, b, load, w, 2, end - 2)
    sweep(b, a, load, w, 3, end - 3)
    piece = rows // CHUNKS

    def put(source, hbm, at, sem):
        copy = pltpu.make_async_copy(
            source.at[pl.ds(FINE + at, piece), fine_own, :],
            hbm.at[pl.ds(at, piece), :, layers],
            sem,
        )
        copy.start()
        return copy

    puts = [put(a, u_hbm, c * piece, sems.at[c]) for c in range(CHUNKS)]

    def remains(i, carry):
        up, here = carry
        down = a[FINE + i + 1]
        around = (up + down) + (roll(here, 1, 0) + roll(here, -1, 0))
        value = lax.slice_in_dim(load[FINE + i] + around, TILE, TILE + columns, axis=0)
        mine = lax.slice_in_dim(here, TILE, TILE + columns, axis=0)
        b[FINE + i, fine_own, :] = value - (4.0 + m_own[i]) * mine
        return here, down

    carry = (a[FINE - 1], a[FINE])
    for c in range(CHUNKS):
        carry = lax.fori_loop(c * piece, (c + 1) * piece, remains, carry, unroll=2)
        puts.append(put(b, d_hbm, c * piece, sems.at[CHUNKS + c]))
    for copy in puts:
        copy.wait()


def call(kernel, chain, outs, args, limit, scratch=(), sems=0, hbm=0, hbm_out=False, aliases=None, extra=0, us=1):
    far, near = pl.BlockSpec(memory_space=pltpu.HBM), pl.BlockSpec(memory_space=pltpu.VMEM)
    near_count = len(args) - hbm - extra
    return pl.pallas_call(
        functools.partial(kernel, chain),
        in_specs=[far] * hbm + [near] * near_count + [far] * extra,
        out_specs=[far if hbm_out else near] * len(outs),
        out_shape=[jax.ShapeDtypeStruct(s, jnp.float32) for s in outs],
        scratch_shapes=[pltpu.VMEM(s + (LANES,), jnp.float32) for s in scratch]
        + ([pltpu.SemaphoreType.DMA((sems,))] if sems else []),
        input_output_aliases=aliases or {},
        cost_estimate=pl.CostEstimate(flops=us * COST, bytes_accessed=0, transcendentals=0),
        compiler_params=pltpu.CompilerParams(vmem_limit_bytes=limit * 1024 * 1024),
    )(*args)


def program(f, u, m):
    rows, columns, layers = f.shape
    half_rows, half_columns = rows // 2, columns // 2
    end, total = rows + 2 * FINE, half_rows + 2 * DEEP
    wide, half_wide = columns + 2 * TILE, half_columns + 2 * TILE
    groups = layers // LANES
    block, coarse_block = (rows, columns, LANES), (half_rows, half_columns, LANES)
    chains = range(groups)

    strip, lane = (10, columns, LANES), (rows, TILE, LANES)
    fines, fine_lanes = [], []

    def send(strips):
        fines.append(swap("band", *strips[:2]))
        fine_lanes.append(swap("lane", *strips[2:]))

    first = call(
        first_kernel, 0, ([strip] * 2 + [lane] * 2) * (groups - 1), (u, f, m), FAR,
        scratch=[(groups - 1, 6, rows, TILE)], sems=12 * (groups - 1), hbm=3, us=4,
    )
    for c in range(groups - 1):
        send(first[4 * c : 4 * c + 4])
    *owns, mass, m_e, m_o, n_e, n_o = call(
        load_kernel, 0,
        [block] * 3 * groups + [(groups,) + coarse_block]
        + [(10 + groups * DEEP // 2, columns, LANES)] * 2 + [(rows + groups * half_rows, TILE, LANES)] * 2,
        (u, f, m), LOAD, scratch=[(half_rows, columns)], sems=3 * groups, hbm=3, us=8,
    )
    send((m_e, m_o, n_e, n_o))
    masses, mass_lanes = fines[-1], fine_lanes[-1]
    owns = [owns[3 * c : 3 * c + 3] for c in chains]
    fine_corners, values, loads, coarses = [], [], [], []
    for c in chains:
        strips = call(
            fine_corner_kernel, c, [(2 * CORNER, TILE, LANES)] * 2, (*owns[c], *fines[c], *loads), 4
        )
        fine_corners.append(swap("lane", *strips))
        v, load, *strips = call(
            before_kernel, c,
            [(end, wide, LANES), coarse_block] + [(DEEP + 4, half_columns, LANES)] * 2,
            (*owns[c], *fines[c], *fine_lanes[c], *fine_corners[c]), 16, us=6,
            scratch=[(end, wide)] * 4 + [(half_rows, columns)],
        )
        values.append(v)
        loads.append(load)
        coarses.append(swap("band", *strips))
    coarse_lanes = []
    lane_rows = half_rows + end // 4 + 2 * DEEP - 1
    for c in chains:
        strips = call(
            coarse_pack_kernel, c, [(lane_rows, TILE, LANES)] * 2, (loads[c], values[c], *coarses[c], *masses, *loads[c + 1 :]), 4
        )
        coarse_lanes.append(swap("lane", *strips))
    fields, xs, nexts = [], [], []
    for c in chains:
        fields.append((loads[c], mass, *coarses[c], *masses, *coarse_lanes[c], *mass_lanes))
        x, *strips = call(
            coarse_kernel, c, [coarse_block] + [(SECOND, half_columns, LANES)] * 2,
            fields[c], 8, us=4, scratch=[(total, half_wide)] * 4,
        )
        xs.append(x)
        nexts.append(swap("band", *strips))
    next_lanes = []
    for c in chains:
        strips = call(
            value_pack_kernel, c, [(half_rows + DEEP - 1, TILE, LANES)] * 2, (xs[c], *nexts[c], *xs[c + 1 :]), 4
        )
        next_lanes.append(swap("lane", *strips))
    results = ()
    for c in chains:
        args = (
            *owns[c][1:], values[c], xs[c], *fines[c], *fine_lanes[c], *fine_corners[c],
            *fields[c], *nexts[c], *next_lanes[c],
        )
        results = tuple(
            call(
                after_kernel, c, [(rows, columns, layers)] * 2, args + results, 20, us=8,
                scratch=[(end, wide)] * 4 + [(total, half_wide)] * 4 + [(half_rows + 4, wide)],
                sems=2 * CHUNKS, hbm_out=True, extra=len(results),
                aliases={len(args) + k: k for k in range(len(results))},
            )
        )
    return results


def solution(mesh):
    return jax.shard_map(
        program,
        mesh=mesh,
        in_specs=(P("band", "lane", None), P("band", "lane", None), P("band", "lane", None)),
        out_specs=(P("band", "lane", None), P("band", "lane", None)),
        check_vma=False,
    )
```

```python
import functools

import jax
import jax.numpy as jnp
from jax import lax
from jax.experimental import pallas as pl
from jax.experimental.pallas import tpu as pltpu
from jax.sharding import PartitionSpec as P


LANES = 128
INNER = 13
FINE = 4
TILE = 8
DEEP = 8
SECOND = 6
FIRST_SWEEPS = DEEP + 1
LAST_SWEEPS = INNER - FIRST_SWEEPS
CHUNKS = 4
FAR = 60
LOAD = 39
COST = 500_000_000


def swaps(count, first):
    pairs = []
    for i in range(first, count - 1, 2):
        pairs += [(i, i + 1), (i + 1, i)]
    return pairs


def swap(axis, even, odd):
    count = lax.axis_size(axis)
    return (
        lax.ppermute(even, axis, swaps(count, 0)),
        lax.ppermute(odd, axis, swaps(count, 1)),
    )


def place(axis):
    at, count = lax.axis_index(axis), lax.axis_size(axis)
    return lax.rem(at, 2) == 0, at > 0, at < count - 1


def roll(value, shift, axis):
    return pltpu.roll(value, shift % value.shape[axis], axis)


def sublane(value):
    return lax.broadcasted_iota(jnp.int32, value.shape, value.ndim - 2)


def by_side(even, got_even, got_odd):
    low = jnp.where(even, got_odd, got_even)
    high = jnp.where(even, got_even, got_odd)
    return low, high


def weight(mass, inside):
    return jnp.where(inside, 0.8 / (4.0 + mass), 0.0)


def new_value(here, left, right, up, down, load, w):
    return 0.2 * here + w * (load + ((up + down) + (left + right)))


def edges(even, rows, depth):
    return jnp.where(even, rows - depth, 0), jnp.where(even, 0, rows - depth)


def packed(u, f, m, v, side):
    s = sublane(u)
    if side:
        f_m = jnp.where(s >= 2, roll(f, -4, 1), roll(m, -6, 1))
        return jnp.where(s >= 6, u, jnp.where(s >= 4, roll(v, -1, 1), f_m))
    f_m = jnp.where(s < 6, roll(f, 4, 1), roll(m, 6, 1))
    return jnp.where(s < 2, u, jnp.where(s < 4, roll(v, 1, 1), f_m))


def swept(u, f, w):
    zero = jnp.zeros((1,) + u.shape[1:], jnp.float32)
    up = jnp.concatenate([zero, u[:-1]], axis=0)
    down = jnp.concatenate([u[1:], zero], axis=0)
    return new_value(u, roll(u, 1, 1), roll(u, -1, 1), up, down, f, w)


def put_sides(even, make, even_ref, odd_ref):
    low, high = make(0), make(1)
    even_ref[...] = jnp.where(even, high, low)
    odd_ref[...] = jnp.where(even, low, high)


def first_kernel(chain, u_hbm, f_hbm, m_hbm, *refs):
    even_b, even_l = place("band")[0], place("lane")[0]
    rows, columns, _ = m_hbm.shape
    arrays = (u_hbm, f_hbm, m_hbm)
    outs, (tiles, sems) = refs[:-2], refs[-2:]
    groups = len(outs) // 4
    tile_copies, copies = [], []
    for g in range(groups):
        at = pl.ds(g * LANES, LANES)
        for side in range(2):
            for part, hbm in enumerate(arrays):
                copy = pltpu.make_async_copy(
                    hbm.at[:, pl.ds(side * (columns - TILE), TILE), at],
                    tiles.at[g, 3 * side + part],
                    sems.at[12 * g + 3 * side + part],
                )
                copy.start()
                tile_copies.append(copy)
        for side, target in enumerate(outs[4 * g : 4 * g + 2]):
            for part, (hbm, depth, first) in enumerate(zip(arrays, (4, 3, 3), (0, 4, 7))):
                start = edges(even_b, rows, depth)[side]
                copy = pltpu.make_async_copy(
                    hbm.at[pl.ds(start, depth), :, at],
                    target.at[pl.ds(first, depth)],
                    sems.at[12 * g + 6 + 3 * side + part],
                )
                copy.start()
                copies.append(copy)
    for g in range(groups):
        for copy in tile_copies[6 * g : 6 * g + 6]:
            copy.wait()

        def make(side, g=g):
            u, f, m = [tiles[g, 3 * side + part] for part in range(3)]
            return packed(u, f, m, swept(u, f, 0.8 / (4.0 + m)), side)

        put_sides(even_l, make, *outs[4 * g + 2 : 4 * g + 4])
    for copy in copies:
        copy.wait()


def mass_place(group, k, half):
    return 10 + group * (DEEP // 2) + k // 2, k % 2 * half


def mass_strip(ref, group, start, width, half):
    places = [mass_place(group, k, half) for k in range(DEEP)]
    return jnp.concatenate([ref[r, pl.ds(c + start, width), :][None] for r, c in places], axis=0)


def load_kernel(chain, u_hbm, f_hbm, m_hbm, *refs):
    even_b, even_l = place("band")[0], place("lane")[0]
    owns, (mass_ref, even_ref, odd_ref, lane_e, lane_o, pairs, sems) = refs[:-7], refs[-7:]
    groups, half_rows, half = mass_ref.shape[0], mass_ref.shape[1], mass_ref.shape[2]
    rows, columns = 2 * half_rows, 2 * half
    even_columns, odd_columns = pl.ds(0, half, 2), pl.ds(1, half, 2)
    copies = [None] * len(owns)
    for g in reversed(range(groups)):
        for part, hbm in ((2, m_hbm), (1, f_hbm), (0, u_hbm)):
            k = 3 * g + part
            copies[k] = pltpu.make_async_copy(hbm.at[:, :, pl.ds(g * LANES, LANES)], owns[k], sems.at[k])
            copies[k].start()
    for g in reversed(range(groups)):
        m_ref = owns[3 * g + 2]
        copies[3 * g + 2].wait()

        def restrict(k, _, g=g, m_ref=m_ref):
            pairs[k] = m_ref[2 * k] + m_ref[2 * k + 1]
            mass_ref[g, k] = 0.5 * (pairs[k, even_columns, :] + pairs[k, odd_columns, :])
            return 0

        lax.fori_loop(0, half_rows, restrict, 0, unroll=2)
        for side, target in enumerate((even_ref, odd_ref)):
            start = edges(even_b, half_rows, DEEP)[side]
            for k in range(DEEP):
                r, c = mass_place(g, k, half)
                target[r, pl.ds(c, half), :] = mass_ref[g, start + k]
    own = owns[3 * groups - 3 :]
    for copy in copies[3 * groups - 3 : 3 * groups - 1]:
        copy.wait()
    for side, target in enumerate((even_ref, odd_ref)):
        for ref, depth, at in zip(own, (4, 3, 3), (0, 4, 7)):
            target[pl.ds(at, depth)] = ref[pl.ds(edges(even_b, rows, depth)[side], depth)]

    def make(side):
        at = pl.ds(side * (columns - TILE), TILE)
        u, f, m = [ref[:, at, :] for ref in own]
        at = pl.ds(side * (half - TILE), TILE)
        parts = [packed(u, f, m, swept(u, f, 0.8 / (4.0 + m)), side)]
        return jnp.concatenate(parts + [mass_ref[g, :, at, :] for g in range(groups)], axis=0)

    put_sides(even_l, make, lane_e, lane_o)
    for g in range(groups - 1):
        for copy in copies[3 * g : 3 * g + 2]:
            copy.wait()


def fold(low, high, side):
    depth = DEEP
    s = sublane(low[0])
    merged = []
    for r in range(1, depth):
        if side:
            merged.append(jnp.where(s >= depth - r, low[r], roll(high[r - 1], -r, 0))[None])
        else:
            merged.append(jnp.where(s < r, low[r], roll(high[r - 1], r, 0))[None])
    return jnp.concatenate(merged, axis=0)


def unfold(got_e, got_o, corner_e, corner_o, even, rows, write):
    def own(k, _):
        low, high = by_side(even, got_e(k), got_o(k))
        write(DEEP + k, low, high)
        return 0

    lax.fori_loop(0, rows, own, 0, unroll=4)
    for r in range(1, DEEP):
        low, high = by_side(even, corner_e(r - 1), corner_o(r - 1))
        write(r, low, high)
        write(DEEP + rows - 1 + r, roll(low, r, 0), roll(high, -r, 0))


CORNER = FINE + 1


def fine_corner_kernel(chain, u_ref, f_ref, m_ref, got_e, got_o, *refs):
    even_ref, odd_ref = refs[-2:]
    even_b, low_b, high_b = place("band")
    rows, columns = u_ref.shape[0], u_ref.shape[1]
    zero = jnp.zeros((1, TILE, LANES), jnp.float32)

    def make(side):
        at = pl.ds(side * (columns - TILE), TILE)
        low, high = by_side(even_b, got_e[:, at, :], got_o[:, at, :])
        parts = []
        for top, inside, halo in ((True, low_b, low), (False, high_b, high)):
            near = pl.ds(0 if top else rows - 2, 2)
            own = [ref[near, at, :] for ref in (u_ref, f_ref, m_ref)]
            h = [halo[:4], halo[4:7], halo[7:10]]
            if top:
                u, f, m = (
                    jnp.concatenate([h[0], own[0]], axis=0),
                    jnp.concatenate([zero, h[1], own[1]], axis=0),
                    jnp.concatenate([zero, h[2], own[2]], axis=0),
                )
            else:
                u, f, m = (
                    jnp.concatenate([own[0], h[0]], axis=0),
                    jnp.concatenate([own[1], h[1], zero], axis=0),
                    jnp.concatenate([own[2], h[2], zero], axis=0),
                )
            w = 0.8 / (4.0 + m)
            if top:
                w = jnp.concatenate([jnp.where(inside, w[:4], 0.0), w[4:]], axis=0)
            else:
                w = jnp.concatenate([w[:2], jnp.where(inside, w[2:], 0.0)], axis=0)
            message = packed(u, f, m, swept(u, f, w), side)
            parts.append(message[:CORNER] if top else message[1:])
        return jnp.concatenate(parts, axis=0)

    put_sides(place("lane")[0], make, even_ref, odd_ref)


def fine_lane_rows(rows, lanes, even, write):
    lane_e, lane_o, corner_e, corner_o = lanes

    def own(r, _):
        low, high = by_side(even, lane_e[r - FINE], lane_o[r - FINE])
        write(r, low, high)
        return 0

    for k in range(CORNER):
        for r, at in ((k, k), (rows + FINE - 1 + k, CORNER + k)):
            low, high = by_side(even, corner_e[at], corner_o[at])
            write(r, low, high)
    lax.fori_loop(CORNER, rows + FINE - 1, own, 0, unroll=2)


def fine_halo(rows, columns, got_e, got_o, lanes, load, w):
    even_b, low_b, high_b = place("band")
    even_l, low_l, high_l = place("lane")
    own = pl.ds(TILE, columns)
    low_rows, high_rows = by_side(even_b, got_e[4:10], got_o[4:10])
    load[1:4, own, :] = low_rows[:3]
    w[1:4, own, :] = weight(low_rows[3:], low_b)
    load[pl.ds(FINE + rows, 3), own, :] = high_rows[:3]
    w[pl.ds(FINE + rows, 3), own, :] = weight(high_rows[3:], high_b)

    def write(r, low, high):
        s = sublane(low)
        inside_row = ((r >= FINE) | low_b) & ((r < FINE + rows) | high_b)
        load[r, pl.ds(0, TILE), :] = roll(low, 4, 0)
        load[r, pl.ds(TILE + columns, TILE), :] = roll(high, -4, 0)
        w[r, pl.ds(0, TILE), :] = weight(roll(low, 6, 0), (s >= 6) & inside_row & low_l)
        w[r, pl.ds(TILE + columns, TILE), :] = weight(
            roll(high, -6, 0), (s < 2) & inside_row & high_l
        )

    fine_lane_rows(rows, lanes, even_l, write)


def own_fields(f_ref, m_ref, load, w):
    rows, columns = m_ref.shape[0], m_ref.shape[1]
    own = pl.ds(TILE, columns)

    def row(r, _):
        load[FINE + r, own, :] = f_ref[r]
        w[FINE + r, own, :] = 0.8 / (4.0 + m_ref[r])
        return 0

    lax.fori_loop(0, rows, row, 0, unroll=2)


def sweep(source, target, load, w, first, last):
    def row(r, carry):
        up, here = carry
        down = source[r + 1]
        target[r] = new_value(here, roll(here, 1, 0), roll(here, -1, 0), up, down, load[r], w[r])
        return here, down

    lax.fori_loop(first, last, row, (source[first - 1], source[first]), unroll=2)


def before_kernel(
    chain, u_ref, f_ref, m_own, got_e, got_o, lane_e, lane_o, corner_e, corner_o,
    v_ref, load_ref, even_ref, odd_ref, load, w, a, b, pairs,
):
    even_b, even_l = place("band")[0], place("lane")[0]
    rows, columns = m_own.shape[0], m_own.shape[1]
    half_columns = columns // 2
    own = pl.ds(TILE, columns)
    left, right = pl.ds(0, TILE), pl.ds(TILE + columns, TILE)
    lanes = (lane_e, lane_o, corner_e, corner_o)
    own_fields(f_ref, m_own, load, w)
    fine_halo(rows, columns, got_e, got_o, lanes, load, w)
    low_rows, high_rows = by_side(even_b, got_e[:4], got_o[:4])
    a[:4, own, :] = low_rows
    a[pl.ds(FINE + rows, 4), own, :] = high_rows

    def copy_row(r, _):
        a[FINE + r, own, :] = u_ref[r]
        return 0

    lax.fori_loop(0, rows, copy_row, 0, unroll=2)

    def put_lane(r, low, high):
        a[r, left, :] = low
        a[r, right, :] = high

    fine_lane_rows(rows, lanes, even_l, put_lane)
    end = rows + 2 * FINE
    sweep(a, b, load, w, 1, end - 1)

    def mend(r, low, high):
        s = sublane(low)
        b[r, left, :] = jnp.where(s == 7, b[r, left, :], roll(low, 1, 0))
        b[r, right, :] = jnp.where(s == 0, b[r, right, :], roll(high, -1, 0))

    fine_lane_rows(rows, lanes, even_l, mend)
    sweep(b, a, load, w, 2, end - 2)
    sweep(a, b, load, w, 3, end - 3)

    def defect_of(i, up, here, down):
        around = (up + down) + (roll(here, 1, 0) + roll(here, -1, 0))
        value = lax.slice_in_dim(load[FINE + i] + around, TILE, TILE + columns, axis=0)
        mine = lax.slice_in_dim(here, TILE, TILE + columns, axis=0)
        return value - (4.0 + m_own[i]) * mine

    even_columns, odd_columns = pl.ds(0, half_columns, 2), pl.ds(1, half_columns, 2)

    def restrict(k, carry):
        up, here = carry
        i = 2 * k
        middle, down = b[FINE + i + 1], b[FINE + i + 2]
        first = defect_of(i, up, here, middle)
        second = defect_of(i + 1, here, middle, down)
        v_ref[FINE + i] = here
        v_ref[FINE + i + 1] = middle
        pairs[k] = first + second
        load_ref[k] = 0.5 * (pairs[k, even_columns, :] + pairs[k, odd_columns, :])
        return middle, down

    lax.fori_loop(0, rows // 2, restrict, (b[FINE - 1], b[FINE]))
    v_ref[FINE - 1] = b[FINE - 1]
    v_ref[FINE + rows] = b[FINE + rows]
    for r in range(FINE - 1):
        v_ref[r] = jnp.zeros_like(b[0])
        v_ref[end - 1 - r] = jnp.zeros_like(b[0])
    for side, target in enumerate((even_ref, odd_ref)):
        start = edges(even_b, rows // 2, DEEP)[side]
        target[:DEEP] = load_ref[pl.ds(start, DEEP)]
        start = FINE + (jnp.where(even_b, rows - 3, 1) if side == 0 else jnp.where(even_b, 1, rows - 3))
        for k in range(4):
            at = pl.ds(TILE + k % 2 * half_columns, half_columns)
            target[DEEP + k] = v_ref[start + k // 2, at, :]


def coarse_pack_kernel(chain, load_ref, v_ref, got_e, got_o, mass_e, mass_o, *refs):
    even_ref, odd_ref = refs[-2:]
    even_b, even_l = place("band")[0], place("lane")[0]
    half, columns = got_e.shape[1], v_ref.shape[1] - 2 * TILE

    def make(side):
        at = pl.ds(side * (half - TILE), TILE)
        tile = pl.ds(TILE + side * (columns - TILE), TILE)
        quarter, first = v_ref.shape[0] // 4, 5 if side else 1
        turned = [
            roll(v_ref[pl.ds(g * quarter, quarter), tile, :], 2 * g - first, 1) for g in range(4)
        ]
        s = sublane(turned[0])
        v = jnp.where(
            s < 4, jnp.where(s < 2, turned[0], turned[1]), jnp.where(s < 6, turned[2], turned[3])
        )
        low, high = by_side(even_b, got_e[:, at, :], got_o[:, at, :])
        load = fold(low[:DEEP], high[:DEEP], side)
        below, above = low[DEEP + 2 + side], high[DEEP + side]
        s = sublane(below)
        keep = s >= 4 if side else s < 4
        second = jnp.where(keep, below, roll(above, 4, 0))[None]
        start = side * (half - TILE)
        low, high = by_side(
            even_b, *[mass_strip(ref, chain, start, TILE, half) for ref in (mass_e, mass_o)]
        )
        return jnp.concatenate([load_ref[:, at, :], v, load, fold(low, high, side), second], axis=0)

    put_sides(even_l, make, even_ref, odd_ref)


def coarse_fields(
    group, load_ref, mass_ref, load_e, load_o, mass_e, mass_o, load_lane_e, load_lane_o, mass_lane_e, mass_lane_o, load, w
):
    even_b, low_b, high_b = place("band")
    even_l, low_l, high_l = place("lane")
    rows, columns = load_ref.shape[0], load_ref.shape[1]
    own = pl.ds(TILE, columns)

    def copy_row(r, _):
        load[DEEP + r, own, :] = load_ref[r]
        w[DEEP + r, own, :] = 0.8 / (4.0 + mass_ref[group, r])
        return 0

    lax.fori_loop(0, rows, copy_row, 0, unroll=4)
    low, high = by_side(even_b, load_e[:DEEP], load_o[:DEEP])
    load[:DEEP, own, :] = low
    load[pl.ds(DEEP + rows, DEEP), own, :] = high
    low, high = by_side(
        even_b, *[mass_strip(ref, group, 0, columns, columns) for ref in (mass_e, mass_o)]
    )
    w[:DEEP, own, :] = weight(low, low_b)
    w[pl.ds(DEEP + rows, DEEP), own, :] = weight(high, high_b)
    left, right = pl.ds(0, TILE), pl.ds(TILE + columns, TILE)

    def put_load(r, low, high):
        load[r, left, :] = low
        load[r, right, :] = high

    def put_weight(r, low, high):
        inside_row = ((r >= DEEP) | low_b) & ((r < DEEP + rows) | high_b)
        w[r, left, :] = weight(low, inside_row & low_l)
        w[r, right, :] = weight(high, inside_row & high_l)

    first = load_lane_e.shape[0] - 2 * DEEP + 1
    second = first + DEEP - 1
    base = (2 + group) * rows
    unfold(
        lambda k: load_lane_e[k], lambda k: load_lane_o[k],
        lambda k: load_lane_e[first + k], lambda k: load_lane_o[first + k], even_l, rows, put_load,
    )
    unfold(
        lambda k: mass_lane_e[base + k], lambda k: mass_lane_o[base + k],
        lambda k: load_lane_e[second + k], lambda k: load_lane_o[second + k], even_l, rows, put_weight,
    )
    zero = jnp.zeros((TILE, LANES), jnp.float32)
    for r in (0, rows + 2 * DEEP - 1):
        put_load(r, zero, zero)
        w[r, left, :] = zero
        w[r, right, :] = zero


def coarse_kernel(chain, *refs):
    fields, (x_ref, even_ref, odd_ref, load, w, a, b) = refs[:10], refs[10:]
    rows, columns = x_ref.shape[0], x_ref.shape[1]
    coarse_fields(chain, *fields, load, w)
    total = rows + 2 * DEEP

    def first(r, _):
        a[r] = w[r] * load[r]
        return 0

    lax.fori_loop(0, total, first, 0, unroll=4)
    source, target = a, b
    for step in range(1, FIRST_SWEEPS):
        sweep(source, target, load, w, step, total - step)
        source, target = target, source

    def out(r, _):
        x_ref[r] = source[DEEP + r, pl.ds(TILE, columns), :]
        return 0

    lax.fori_loop(0, rows, out, 0, unroll=4)
    for side, target in enumerate((even_ref, odd_ref)):
        start = edges(place("band")[0], rows, SECOND)[side]
        target[...] = x_ref[pl.ds(start, SECOND)]


def value_pack_kernel(chain, x_ref, got_e, got_o, *refs):
    even_ref, odd_ref = refs[-2:]
    even_b, even_l = place("band")[0], place("lane")[0]
    zero = jnp.zeros((DEEP - SECOND, TILE, LANES), jnp.float32)

    def make(side):
        at = pl.ds(side * (got_e.shape[1] - TILE), TILE)
        low, high = by_side(even_b, got_e[:, at, :], got_o[:, at, :])
        low, high = jnp.concatenate([zero, low], axis=0), jnp.concatenate([high, zero], axis=0)
        return jnp.concatenate([x_ref[:, at, :], fold(low, high, side)], axis=0)

    put_sides(even_l, make, even_ref, odd_ref)


def after_kernel(
    chain, m_own, v_ref, x_ref, load, w, coarse_load, coarse_w,
    coarse_e, coarse_o, coarse_lane_e, coarse_lane_o,
    value_e, value_o, value_lane_e, value_lane_o, *rest,
):
    u_hbm, d_hbm, a, b, x, y, spread, sems = rest[-8:]
    even_b, even_l = place("band")[0], place("lane")[0]
    rows, columns = m_own.shape[0], m_own.shape[1]
    half_rows, half_columns = rows // 2, columns // 2
    layers = pl.ds(chain * LANES, LANES)
    fine_own = pl.ds(TILE, columns)
    left, right = pl.ds(0, TILE), pl.ds(TILE + columns, TILE)
    own = pl.ds(TILE, half_columns)
    total = half_rows + 2 * DEEP
    low, high = by_side(even_b, value_e[...], value_o[...])
    x[DEEP - SECOND : DEEP, own, :] = low
    x[pl.ds(DEEP + half_rows, SECOND), own, :] = high

    def coarse_copy(r, _):
        x[DEEP + r, own, :] = x_ref[r]
        return 0

    lax.fori_loop(0, half_rows, coarse_copy, 0, unroll=4)

    def put_value(r, low, high):
        x[r, pl.ds(0, TILE), :] = low
        x[r, pl.ds(TILE + half_columns, TILE), :] = high

    unfold(
        lambda k: value_lane_e[k], lambda k: value_lane_o[k],
        lambda k: value_lane_e[half_rows + k], lambda k: value_lane_o[half_rows + k], even_l, half_rows, put_value,
    )
    source, target = x, y
    for step in range(1, LAST_SWEEPS + 1):
        edge = DEEP - SECOND + step
        sweep(source, target, coarse_load, coarse_w, edge, total - edge)
        source, target = target, source

    a[FINE - 1] = v_ref[FINE - 1]
    a[FINE + rows] = v_ref[FINE + rows]
    for i in range(2):
        for part in range(2):
            at = pl.ds(TILE + part * half_columns, half_columns)
            k = DEEP + 2 * i + part
            low, high = by_side(even_b, coarse_e[k], coarse_o[k])
            a[1 + i, at, :] = low
            a[FINE + rows + 1 + i, at, :] = high
    end = rows + 2 * FINE
    quarter = end // 4
    first = half_rows

    def fine_lane(k, _):
        low, high = by_side(even_l, coarse_lane_e[first + k], coarse_lane_o[first + k])
        s = sublane(low)
        for g in range(4):
            r = g * quarter + k
            a[r, left, :] = jnp.where(s == TILE - 1, v_ref[r, left, :], roll(low, 5 - 2 * g, 0))
            a[r, right, :] = jnp.where(s == 0, v_ref[r, right, :], roll(high, 1 - 2 * g, 0))
        return 0

    lax.fori_loop(0, quarter, fine_lane, 0, unroll=2)
    at = coarse_lane_e.shape[0] - 1
    low, high = by_side(even_l, coarse_lane_e[at], coarse_lane_o[at])
    for r, turn in ((FINE - 2, 0), (FINE + rows + 1, 4)):
        a[r, left, :] = roll(low, turn, 0)
        a[r, right, :] = roll(high, turn, 0)
    across = columns // 2 + TILE
    skip = TILE - TILE // 2

    def spread_row(k):
        value = source[DEEP - 2 + k, pl.ds(skip, across), :]
        spread[k, pl.ds(0, across, 2), :] = value
        spread[k, pl.ds(1, across, 2), :] = value
        return spread[k]

    for k in (0, 1, half_rows + 2, half_rows + 3):
        both = spread_row(k)
        a[2 * k] += both
        a[2 * k + 1] += both

    def correct(k, _):
        both = spread_row(k)
        ends = [lax.slice_in_dim(both, s, s + TILE, axis=0) for s in (0, TILE + columns)]
        middle = lax.slice_in_dim(both, TILE, TILE + columns, axis=0)
        for part in range(2):
            r = 2 * k + part
            a[r, fine_own, :] = v_ref[r, fine_own, :] + middle
            a[r, left, :] += ends[0]
            a[r, right, :] += ends[1]
        return 0

    lax.fori_loop(2, half_rows + 2, correct, 0, unroll=2)
    sweep(a, b, load, w, 2, end - 2)
    sweep(b, a, load, w, 3, end - 3)
    piece = rows // CHUNKS

    def put(source, hbm, at, sem):
        copy = pltpu.make_async_copy(
            source.at[pl.ds(FINE + at, piece), fine_own, :],
            hbm.at[pl.ds(at, piece), :, layers],
            sem,
        )
        copy.start()
        return copy

    puts = [put(a, u_hbm, c * piece, sems.at[c]) for c in range(CHUNKS)]

    def remains(i, carry):
        up, here = carry
        down = a[FINE + i + 1]
        around = (up + down) + (roll(here, 1, 0) + roll(here, -1, 0))
        value = lax.slice_in_dim(load[FINE + i] + around, TILE, TILE + columns, axis=0)
        mine = lax.slice_in_dim(here, TILE, TILE + columns, axis=0)
        b[FINE + i, fine_own, :] = value - (4.0 + m_own[i]) * mine
        return here, down

    carry = (a[FINE - 1], a[FINE])
    for c in range(CHUNKS):
        carry = lax.fori_loop(c * piece, (c + 1) * piece, remains, carry, unroll=2)
        puts.append(put(b, d_hbm, c * piece, sems.at[CHUNKS + c]))
    for copy in puts:
        copy.wait()


def call(kernel, chain, outs, args, limit, scratch=(), sems=0, hbm=0, hbm_out=False, aliases=None, extra=0, us=1):
    far, near = pl.BlockSpec(memory_space=pltpu.HBM), pl.BlockSpec(memory_space=pltpu.VMEM)
    near_count = len(args) - hbm - extra
    return pl.pallas_call(
        functools.partial(kernel, chain),
        in_specs=[far] * hbm + [near] * near_count + [far] * extra,
        out_specs=[far if hbm_out else near] * len(outs),
        out_shape=[jax.ShapeDtypeStruct(s, jnp.float32) for s in outs],
        scratch_shapes=[pltpu.VMEM(s + (LANES,), jnp.float32) for s in scratch]
        + ([pltpu.SemaphoreType.DMA((sems,))] if sems else []),
        input_output_aliases=aliases or {},
        cost_estimate=pl.CostEstimate(flops=us * COST, bytes_accessed=0, transcendentals=0),
        compiler_params=pltpu.CompilerParams(vmem_limit_bytes=limit * 1024 * 1024),
    )(*args)


def program(f, u, m):
    rows, columns, layers = f.shape
    half_rows, half_columns = rows // 2, columns // 2
    end, total = rows + 2 * FINE, half_rows + 2 * DEEP
    wide, half_wide = columns + 2 * TILE, half_columns + 2 * TILE
    groups = layers // LANES
    block, coarse_block = (rows, columns, LANES), (half_rows, half_columns, LANES)
    chains = range(groups)

    strip, lane = (10, columns, LANES), (rows, TILE, LANES)
    fines, fine_lanes = [], []

    def send(strips):
        fines.append(swap("band", *strips[:2]))
        fine_lanes.append(swap("lane", *strips[2:]))

    first = call(
        first_kernel, 0, ([strip] * 2 + [lane] * 2) * (groups - 1), (u, f, m), FAR,
        scratch=[(groups - 1, 6, rows, TILE)], sems=12 * (groups - 1), hbm=3, us=4,
    )
    for c in range(groups - 1):
        send(first[4 * c : 4 * c + 4])
    *owns, mass, m_e, m_o, n_e, n_o = call(
        load_kernel, 0,
        [block] * 3 * groups + [(groups,) + coarse_block]
        + [(10 + groups * DEEP // 2, columns, LANES)] * 2 + [(rows + groups * half_rows, TILE, LANES)] * 2,
        (u, f, m), LOAD, scratch=[(half_rows, columns)], sems=3 * groups, hbm=3, us=8,
    )
    send((m_e, m_o, n_e, n_o))
    masses, mass_lanes = fines[-1], fine_lanes[-1]
    owns = [owns[3 * c : 3 * c + 3] for c in chains]
    fine_corners, values, loads, coarses, fields = [], [], [], [], []
    for c in chains:
        strips = call(
            fine_corner_kernel, c, [(2 * CORNER, TILE, LANES)] * 2, (*owns[c], *fines[c], *loads), 4
        )
        fine_corners.append(swap("lane", *strips))
        v, load, *strips, load_wide, w_wide = call(
            before_kernel, c,
            [(end, wide, LANES), coarse_block] + [(DEEP + 4, half_columns, LANES)] * 2
            + [(end, wide, LANES)] * 2,
            (*owns[c], *fines[c], *fine_lanes[c], *fine_corners[c]), 10, us=6,
            scratch=[(end, wide)] * 2 + [(half_rows, columns)],
        )
        fields.append((load_wide, w_wide))
        values.append(v)
        loads.append(load)
        coarses.append(swap("band", *strips))
    coarse_lanes = []
    lane_rows = half_rows + end // 4 + 2 * DEEP - 1
    for c in chains:
        strips = call(
            coarse_pack_kernel, c, [(lane_rows, TILE, LANES)] * 2, (loads[c], values[c], *coarses[c], *masses, *loads[c + 1 :]), 4
        )
        coarse_lanes.append(swap("lane", *strips))
    xs, nexts = [], []
    for c in chains:
        x, *strips, load_wide, w_wide = call(
            coarse_kernel, c,
            [coarse_block] + [(SECOND, half_columns, LANES)] * 2 + [(total, half_wide, LANES)] * 2,
            (loads[c], mass, *coarses[c], *masses, *coarse_lanes[c], *mass_lanes), 6, us=4,
            scratch=[(total, half_wide)] * 2,
        )
        fields[c] += (load_wide, w_wide)
        xs.append(x)
        nexts.append(swap("band", *strips))
    next_lanes = []
    for c in chains:
        strips = call(
            value_pack_kernel, c, [(half_rows + DEEP - 1, TILE, LANES)] * 2, (xs[c], *nexts[c], *xs[c + 1 :]), 4
        )
        next_lanes.append(swap("lane", *strips))
    results = ()
    for c in chains:
        args = (
            owns[c][2], values[c], xs[c], *fields[c], *coarses[c], *coarse_lanes[c], *nexts[c], *next_lanes[c],
        )
        results = tuple(
            call(
                after_kernel, c, [(rows, columns, layers)] * 2, args + results, 12, us=8,
                scratch=[(end, wide)] * 2 + [(total, half_wide)] * 2 + [(half_rows + 4, wide)],
                sems=2 * CHUNKS, hbm_out=True, extra=len(results),
                aliases={len(args) + k: k for k in range(len(results))},
            )
        )
    return results


def solution(mesh):
    return jax.shard_map(
        program,
        mesh=mesh,
        in_specs=(P("band", "lane", None), P("band", "lane", None), P("band", "lane", None)),
        out_specs=(P("band", "lane", None), P("band", "lane", None)),
        check_vma=False,
    )
```

```python
import functools

import jax
import jax.numpy as jnp
from jax import lax
from jax.experimental import pallas as pl
from jax.experimental.pallas import tpu as pltpu
from jax.sharding import PartitionSpec as P


LANES = 128
INNER = 13
FINE = 4
TILE = 8
DEEP = 8
SECOND = 6
FIRST_SWEEPS = DEEP + 1
LAST_SWEEPS = INNER - FIRST_SWEEPS
CHUNKS = 4
FAR = 60
LOAD = 39
COST = 500_000_000


def swaps(count, first):
    pairs = []
    for i in range(first, count - 1, 2):
        pairs += [(i, i + 1), (i + 1, i)]
    return pairs


def swap(axis, even, odd):
    count = lax.axis_size(axis)
    got_even = lax.ppermute(even, axis, swaps(count, 0))
    got_odd = lax.ppermute(odd, axis, swaps(count, 1))
    return got_even, got_odd


def place(axis):
    at, count = lax.axis_index(axis), lax.axis_size(axis)
    return lax.rem(at, 2) == 0, at > 0, at < count - 1


def roll(value, shift, axis):
    return pltpu.roll(value, shift % value.shape[axis], axis)


def sublane(value):
    return lax.broadcasted_iota(jnp.int32, value.shape, value.ndim - 2)


def by_side(even, got_even, got_odd):
    low = jnp.where(even, got_odd, got_even)
    high = jnp.where(even, got_even, got_odd)
    return low, high


def weight(mass, inside):
    return jnp.where(inside, 0.8 / (4.0 + mass), 0.0)


def new_value(here, left, right, up, down, load, w):
    return 0.2 * here + w * (load + ((up + down) + (left + right)))


def edges(even, rows, depth):
    return jnp.where(even, rows - depth, 0), jnp.where(even, 0, rows - depth)


def packed(u, f, m, v, side):
    s = sublane(u)
    if side:
        f_m = jnp.where(s >= 2, roll(f, -4, 1), roll(m, -6, 1))
        return jnp.where(s >= 6, u, jnp.where(s >= 4, roll(v, -1, 1), f_m))
    f_m = jnp.where(s < 6, roll(f, 4, 1), roll(m, 6, 1))
    return jnp.where(s < 2, u, jnp.where(s < 4, roll(v, 1, 1), f_m))


def swept(u, f, w):
    zero = jnp.zeros((1,) + u.shape[1:], jnp.float32)
    up = jnp.concatenate([zero, u[:-1]], axis=0)
    down = jnp.concatenate([u[1:], zero], axis=0)
    return new_value(u, roll(u, 1, 1), roll(u, -1, 1), up, down, f, w)


def put_sides(even, make, even_ref, odd_ref):
    low, high = make(0), make(1)
    even_ref[...] = jnp.where(even, high, low)
    odd_ref[...] = jnp.where(even, low, high)


def first_kernel(chain, u_hbm, f_hbm, m_hbm, *refs):
    even_b, even_l = place("band")[0], place("lane")[0]
    rows, columns, _ = m_hbm.shape
    arrays = (u_hbm, f_hbm, m_hbm)
    outs, (tiles, sems) = refs[:-2], refs[-2:]
    groups = len(outs) // 4
    tile_copies, copies = [], []
    for g in range(groups):
        at = pl.ds(g * LANES, LANES)
        for side in range(2):
            for part, hbm in enumerate(arrays):
                copy = pltpu.make_async_copy(
                    hbm.at[:, pl.ds(side * (columns - TILE), TILE), at],
                    tiles.at[g, 3 * side + part],
                    sems.at[12 * g + 3 * side + part],
                )
                copy.start()
                tile_copies.append(copy)
        for side, target in enumerate(outs[4 * g : 4 * g + 2]):
            for part, (hbm, depth, first) in enumerate(zip(arrays, (4, 3, 3), (0, 4, 7))):
                start = edges(even_b, rows, depth)[side]
                copy = pltpu.make_async_copy(
                    hbm.at[pl.ds(start, depth), :, at],
                    target.at[pl.ds(first, depth)],
                    sems.at[12 * g + 6 + 3 * side + part],
                )
                copy.start()
                copies.append(copy)
    for g in range(groups):
        for copy in tile_copies[6 * g : 6 * g + 6]:
            copy.wait()

        def make(side, g=g):
            u, f, m = [tiles[g, 3 * side + part] for part in range(3)]
            return packed(u, f, m, swept(u, f, 0.8 / (4.0 + m)), side)

        put_sides(even_l, make, *outs[4 * g + 2 : 4 * g + 4])
    for copy in copies:
        copy.wait()


def mass_place(group, k, half):
    return 10 + group * (DEEP // 2) + k // 2, k % 2 * half


def mass_strip(ref, group, start, width, half):
    places = [mass_place(group, k, half) for k in range(DEEP)]
    return jnp.concatenate([ref[r, pl.ds(c + start, width), :][None] for r, c in places], axis=0)


def load_kernel(chain, u_hbm, f_hbm, m_hbm, *refs):
    even_b, even_l = place("band")[0], place("lane")[0]
    owns, (mass_ref, even_ref, odd_ref, lane_e, lane_o, pairs, sems) = refs[:-7], refs[-7:]
    groups, half_rows, half = mass_ref.shape[0], mass_ref.shape[1], mass_ref.shape[2]
    rows, columns = 2 * half_rows, 2 * half
    even_columns, odd_columns = pl.ds(0, half, 2), pl.ds(1, half, 2)
    copies = [None] * len(owns)
    for g in reversed(range(groups)):
        for part, hbm in ((2, m_hbm), (1, f_hbm), (0, u_hbm)):
            k = 3 * g + part
            copies[k] = pltpu.make_async_copy(hbm.at[:, :, pl.ds(g * LANES, LANES)], owns[k], sems.at[k])
            copies[k].start()
    for g in reversed(range(groups)):
        m_ref = owns[3 * g + 2]
        copies[3 * g + 2].wait()

        def restrict(k, _, g=g, m_ref=m_ref):
            pairs[k] = m_ref[2 * k] + m_ref[2 * k + 1]
            mass_ref[g, k] = 0.5 * (pairs[k, even_columns, :] + pairs[k, odd_columns, :])
            return 0

        lax.fori_loop(0, half_rows, restrict, 0, unroll=2)
        for side, target in enumerate((even_ref, odd_ref)):
            start = edges(even_b, half_rows, DEEP)[side]
            for k in range(DEEP):
                r, c = mass_place(g, k, half)
                target[r, pl.ds(c, half), :] = mass_ref[g, start + k]
    own = owns[3 * groups - 3 :]
    for copy in copies[3 * groups - 3 : 3 * groups - 1]:
        copy.wait()
    for side, target in enumerate((even_ref, odd_ref)):
        for ref, depth, at in zip(own, (4, 3, 3), (0, 4, 7)):
            target[pl.ds(at, depth)] = ref[pl.ds(edges(even_b, rows, depth)[side], depth)]

    def make(side):
        at = pl.ds(side * (columns - TILE), TILE)
        u, f, m = [ref[:, at, :] for ref in own]
        at = pl.ds(side * (half - TILE), TILE)
        parts = [packed(u, f, m, swept(u, f, 0.8 / (4.0 + m)), side)]
        return jnp.concatenate(parts + [mass_ref[g, :, at, :] for g in range(groups)], axis=0)

    put_sides(even_l, make, lane_e, lane_o)
    for g in range(groups - 1):
        for copy in copies[3 * g : 3 * g + 2]:
            copy.wait()


def fold(low, high, side):
    depth = DEEP
    s = sublane(low[0])
    merged = []
    for r in range(1, depth):
        if side:
            merged.append(jnp.where(s >= depth - r, low[r], roll(high[r - 1], -r, 0))[None])
        else:
            merged.append(jnp.where(s < r, low[r], roll(high[r - 1], r, 0))[None])
    return jnp.concatenate(merged, axis=0)


def unfold(got_e, got_o, corner_e, corner_o, even, rows, write):
    def own(k, _):
        low, high = by_side(even, got_e(k), got_o(k))
        write(DEEP + k, low, high)
        return 0

    lax.fori_loop(0, rows, own, 0, unroll=4)
    for r in range(1, DEEP):
        low, high = by_side(even, corner_e(r - 1), corner_o(r - 1))
        write(r, low, high)
        write(DEEP + rows - 1 + r, roll(low, r, 0), roll(high, -r, 0))


CORNER = FINE + 1


def fine_corner_kernel(chain, u_ref, f_ref, m_ref, got_e, got_o, *refs):
    even_ref, odd_ref = refs[-2:]
    even_b, low_b, high_b = place("band")
    rows, columns = u_ref.shape[0], u_ref.shape[1]
    zero = jnp.zeros((1, TILE, LANES), jnp.float32)

    def make(side):
        at = pl.ds(side * (columns - TILE), TILE)
        low, high = by_side(even_b, got_e[:, at, :], got_o[:, at, :])
        parts = []
        for top, inside, halo in ((True, low_b, low), (False, high_b, high)):
            near = pl.ds(0 if top else rows - 2, 2)
            own = [ref[near, at, :] for ref in (u_ref, f_ref, m_ref)]
            h = [halo[:4], halo[4:7], halo[7:10]]
            if top:
                u, f, m = (
                    jnp.concatenate([h[0], own[0]], axis=0),
                    jnp.concatenate([zero, h[1], own[1]], axis=0),
                    jnp.concatenate([zero, h[2], own[2]], axis=0),
                )
            else:
                u, f, m = (
                    jnp.concatenate([own[0], h[0]], axis=0),
                    jnp.concatenate([own[1], h[1], zero], axis=0),
                    jnp.concatenate([own[2], h[2], zero], axis=0),
                )
            w = 0.8 / (4.0 + m)
            if top:
                w = jnp.concatenate([jnp.where(inside, w[:4], 0.0), w[4:]], axis=0)
            else:
                w = jnp.concatenate([w[:2], jnp.where(inside, w[2:], 0.0)], axis=0)
            message = packed(u, f, m, swept(u, f, w), side)
            parts.append(message[:CORNER] if top else message[1:])
        return jnp.concatenate(parts, axis=0)

    put_sides(place("lane")[0], make, even_ref, odd_ref)


def fine_lane_rows(rows, lanes, even, write):
    lane_e, lane_o, corner_e, corner_o = lanes

    def own(r, _):
        low, high = by_side(even, lane_e[r - FINE], lane_o[r - FINE])
        write(r, low, high)
        return 0

    for k in range(CORNER):
        for r, at in ((k, k), (rows + FINE - 1 + k, CORNER + k)):
            low, high = by_side(even, corner_e[at], corner_o[at])
            write(r, low, high)
    lax.fori_loop(CORNER, rows + FINE - 1, own, 0, unroll=2)


def fine_halo(rows, columns, got_e, got_o, lanes, load, w):
    even_b, low_b, high_b = place("band")
    even_l, low_l, high_l = place("lane")
    own = pl.ds(TILE, columns)
    low_rows, high_rows = by_side(even_b, got_e[4:10], got_o[4:10])
    load[1:4, own, :] = low_rows[:3]
    w[1:4, own, :] = weight(low_rows[3:], low_b)
    load[pl.ds(FINE + rows, 3), own, :] = high_rows[:3]
    w[pl.ds(FINE + rows, 3), own, :] = weight(high_rows[3:], high_b)

    def write(r, low, high):
        s = sublane(low)
        inside_row = ((r >= FINE) | low_b) & ((r < FINE + rows) | high_b)
        load[r, pl.ds(0, TILE), :] = roll(low, 4, 0)
        load[r, pl.ds(TILE + columns, TILE), :] = roll(high, -4, 0)
        w[r, pl.ds(0, TILE), :] = weight(roll(low, 6, 0), (s >= 6) & inside_row & low_l)
        w[r, pl.ds(TILE + columns, TILE), :] = weight(
            roll(high, -6, 0), (s < 2) & inside_row & high_l
        )

    fine_lane_rows(rows, lanes, even_l, write)


def own_fields(f_ref, m_ref, load, w):
    rows, columns = m_ref.shape[0], m_ref.shape[1]
    own = pl.ds(TILE, columns)

    def row(r, _):
        load[FINE + r, own, :] = f_ref[r]
        w[FINE + r, own, :] = 0.8 / (4.0 + m_ref[r])
        return 0

    lax.fori_loop(0, rows, row, 0, unroll=2)


def sweep(source, target, load, w, first, last):
    def row(r, carry):
        up, here = carry
        down = source[r + 1]
        target[r] = new_value(here, roll(here, 1, 0), roll(here, -1, 0), up, down, load[r], w[r])
        return here, down

    lax.fori_loop(first, last, row, (source[first - 1], source[first]), unroll=2)


def before_kernel(
    chain, u_ref, f_ref, m_own, got_e, got_o, lane_e, lane_o, corner_e, corner_o,
    v_ref, load_ref, even_ref, odd_ref, load, w, a, b, pairs,
):
    even_b, even_l = place("band")[0], place("lane")[0]
    rows, columns = m_own.shape[0], m_own.shape[1]
    half_columns = columns // 2
    own = pl.ds(TILE, columns)
    left, right = pl.ds(0, TILE), pl.ds(TILE + columns, TILE)
    lanes = (lane_e, lane_o, corner_e, corner_o)
    own_fields(f_ref, m_own, load, w)
    fine_halo(rows, columns, got_e, got_o, lanes, load, w)
    low_rows, high_rows = by_side(even_b, got_e[:4], got_o[:4])
    a[:4, own, :] = low_rows
    a[pl.ds(FINE + rows, 4), own, :] = high_rows

    def copy_row(r, _):
        a[FINE + r, own, :] = u_ref[r]
        return 0

    lax.fori_loop(0, rows, copy_row, 0, unroll=2)

    def put_lane(r, low, high):
        a[r, left, :] = low
        a[r, right, :] = high

    fine_lane_rows(rows, lanes, even_l, put_lane)
    end = rows + 2 * FINE
    sweep(a, b, load, w, 1, end - 1)

    def mend(r, low, high):
        s = sublane(low)
        b[r, left, :] = jnp.where(s == 7, b[r, left, :], roll(low, 1, 0))
        b[r, right, :] = jnp.where(s == 0, b[r, right, :], roll(high, -1, 0))

    fine_lane_rows(rows, lanes, even_l, mend)
    sweep(b, a, load, w, 2, end - 2)
    sweep(a, b, load, w, 3, end - 3)

    def defect_of(i, up, here, down):
        around = (up + down) + (roll(here, 1, 0) + roll(here, -1, 0))
        value = lax.slice_in_dim(load[FINE + i] + around, TILE, TILE + columns, axis=0)
        mine = lax.slice_in_dim(here, TILE, TILE + columns, axis=0)
        return value - (4.0 + m_own[i]) * mine

    even_columns, odd_columns = pl.ds(0, half_columns, 2), pl.ds(1, half_columns, 2)

    def restrict(k, carry):
        up, here = carry
        i = 2 * k
        middle, down = b[FINE + i + 1], b[FINE + i + 2]
        first = defect_of(i, up, here, middle)
        second = defect_of(i + 1, here, middle, down)
        v_ref[FINE + i] = here
        v_ref[FINE + i + 1] = middle
        pairs[k] = first + second
        load_ref[k] = 0.5 * (pairs[k, even_columns, :] + pairs[k, odd_columns, :])
        return middle, down

    lax.fori_loop(0, rows // 2, restrict, (b[FINE - 1], b[FINE]))
    v_ref[FINE - 1] = b[FINE - 1]
    v_ref[FINE + rows] = b[FINE + rows]
    for r in range(FINE - 1):
        v_ref[r] = jnp.zeros_like(b[0])
        v_ref[end - 1 - r] = jnp.zeros_like(b[0])
    for side, target in enumerate((even_ref, odd_ref)):
        start = edges(even_b, rows // 2, DEEP)[side]
        target[:DEEP] = load_ref[pl.ds(start, DEEP)]
        start = FINE + (jnp.where(even_b, rows - 3, 1) if side == 0 else jnp.where(even_b, 1, rows - 3))
        for k in range(4):
            at = pl.ds(TILE + k % 2 * half_columns, half_columns)
            target[DEEP + k] = v_ref[start + k // 2, at, :]


def coarse_pack_kernel(chain, load_ref, v_ref, got_e, got_o, mass_e, mass_o, *refs):
    even_ref, odd_ref = refs[-2:]
    even_b, even_l = place("band")[0], place("lane")[0]
    half, columns = got_e.shape[1], v_ref.shape[1] - 2 * TILE

    def make(side):
        at = pl.ds(side * (half - TILE), TILE)
        tile = pl.ds(TILE + side * (columns - TILE), TILE)
        quarter, first = v_ref.shape[0] // 4, 5 if side else 1
        turned = [
            roll(v_ref[pl.ds(g * quarter, quarter), tile, :], 2 * g - first, 1) for g in range(4)
        ]
        s = sublane(turned[0])
        v = jnp.where(
            s < 4, jnp.where(s < 2, turned[0], turned[1]), jnp.where(s < 6, turned[2], turned[3])
        )
        low, high = by_side(even_b, got_e[:, at, :], got_o[:, at, :])
        load = fold(low[:DEEP], high[:DEEP], side)
        below, above = low[DEEP + 2 + side], high[DEEP + side]
        s = sublane(below)
        keep = s >= 4 if side else s < 4
        second = jnp.where(keep, below, roll(above, 4, 0))[None]
        start = side * (half - TILE)
        low, high = by_side(
            even_b, *[mass_strip(ref, chain, start, TILE, half) for ref in (mass_e, mass_o)]
        )
        return jnp.concatenate([load_ref[:, at, :], v, load, fold(low, high, side), second], axis=0)

    put_sides(even_l, make, even_ref, odd_ref)


def coarse_fields(
    group, load_ref, mass_ref, load_e, load_o, mass_e, mass_o, load_lane_e, load_lane_o, mass_lane_e, mass_lane_o, load, w
):
    even_b, low_b, high_b = place("band")
    even_l, low_l, high_l = place("lane")
    rows, columns = load_ref.shape[0], load_ref.shape[1]
    own = pl.ds(TILE, columns)

    def copy_row(r, _):
        load[DEEP + r, own, :] = load_ref[r]
        w[DEEP + r, own, :] = 0.8 / (4.0 + mass_ref[group, r])
        return 0

    lax.fori_loop(0, rows, copy_row, 0, unroll=4)
    low, high = by_side(even_b, load_e[:DEEP], load_o[:DEEP])
    load[:DEEP, own, :] = low
    load[pl.ds(DEEP + rows, DEEP), own, :] = high
    low, high = by_side(
        even_b, *[mass_strip(ref, group, 0, columns, columns) for ref in (mass_e, mass_o)]
    )
    w[:DEEP, own, :] = weight(low, low_b)
    w[pl.ds(DEEP + rows, DEEP), own, :] = weight(high, high_b)
    left, right = pl.ds(0, TILE), pl.ds(TILE + columns, TILE)

    def put_load(r, low, high):
        load[r, left, :] = low
        load[r, right, :] = high

    def put_weight(r, low, high):
        inside_row = ((r >= DEEP) | low_b) & ((r < DEEP + rows) | high_b)
        w[r, left, :] = weight(low, inside_row & low_l)
        w[r, right, :] = weight(high, inside_row & high_l)

    first = load_lane_e.shape[0] - 2 * DEEP + 1
    second = first + DEEP - 1
    base = (2 + group) * rows
    unfold(
        lambda k: load_lane_e[k], lambda k: load_lane_o[k],
        lambda k: load_lane_e[first + k], lambda k: load_lane_o[first + k], even_l, rows, put_load,
    )
    unfold(
        lambda k: mass_lane_e[base + k], lambda k: mass_lane_o[base + k],
        lambda k: load_lane_e[second + k], lambda k: load_lane_o[second + k], even_l, rows, put_weight,
    )
    zero = jnp.zeros((TILE, LANES), jnp.float32)
    for r in (0, rows + 2 * DEEP - 1):
        put_load(r, zero, zero)
        w[r, left, :] = zero
        w[r, right, :] = zero


def coarse_kernel(chain, *refs):
    fields, (x_ref, even_ref, odd_ref, load, w, a, b) = refs[:10], refs[10:]
    rows, columns = x_ref.shape[0], x_ref.shape[1]
    coarse_fields(chain, *fields, load, w)
    total = rows + 2 * DEEP

    def first(r, _):
        a[r] = w[r] * load[r]
        return 0

    lax.fori_loop(0, total, first, 0, unroll=4)
    source, target = a, b
    for step in range(1, FIRST_SWEEPS):
        sweep(source, target, load, w, step, total - step)
        source, target = target, source

    def out(r, _):
        x_ref[r] = source[DEEP + r, pl.ds(TILE, columns), :]
        return 0

    lax.fori_loop(0, rows, out, 0, unroll=4)
    for side, target in enumerate((even_ref, odd_ref)):
        start = edges(place("band")[0], rows, SECOND)[side]
        target[...] = x_ref[pl.ds(start, SECOND)]


def value_pack_kernel(chain, x_ref, got_e, got_o, *refs):
    even_ref, odd_ref = refs[-2:]
    even_b, even_l = place("band")[0], place("lane")[0]
    zero = jnp.zeros((DEEP - SECOND, TILE, LANES), jnp.float32)

    def make(side):
        at = pl.ds(side * (got_e.shape[1] - TILE), TILE)
        low, high = by_side(even_b, got_e[:, at, :], got_o[:, at, :])
        low, high = jnp.concatenate([zero, low], axis=0), jnp.concatenate([high, zero], axis=0)
        return jnp.concatenate([x_ref[:, at, :], fold(low, high, side)], axis=0)

    put_sides(even_l, make, even_ref, odd_ref)


def after_kernel(
    chain, m_own, v_ref, x_ref, load, w, coarse_load, coarse_w,
    coarse_e, coarse_o, coarse_lane_e, coarse_lane_o,
    value_e, value_o, value_lane_e, value_lane_o, *rest,
):
    u_hbm, d_hbm, a, b, x, y, spread, sems = rest[-8:]
    even_b, even_l = place("band")[0], place("lane")[0]
    rows, columns = m_own.shape[0], m_own.shape[1]
    half_rows, half_columns = rows // 2, columns // 2
    layers = pl.ds(chain * LANES, LANES)
    fine_own = pl.ds(TILE, columns)
    left, right = pl.ds(0, TILE), pl.ds(TILE + columns, TILE)
    own = pl.ds(TILE, half_columns)
    total = half_rows + 2 * DEEP
    low, high = by_side(even_b, value_e[...], value_o[...])
    x[DEEP - SECOND : DEEP, own, :] = low
    x[pl.ds(DEEP + half_rows, SECOND), own, :] = high

    def coarse_copy(r, _):
        x[DEEP + r, own, :] = x_ref[r]
        return 0

    lax.fori_loop(0, half_rows, coarse_copy, 0, unroll=4)

    def put_value(r, low, high):
        x[r, pl.ds(0, TILE), :] = low
        x[r, pl.ds(TILE + half_columns, TILE), :] = high

    unfold(
        lambda k: value_lane_e[k], lambda k: value_lane_o[k],
        lambda k: value_lane_e[half_rows + k], lambda k: value_lane_o[half_rows + k], even_l, half_rows, put_value,
    )
    source, target = x, y
    for step in range(1, LAST_SWEEPS + 1):
        edge = DEEP - SECOND + step
        sweep(source, target, coarse_load, coarse_w, edge, total - edge)
        source, target = target, source

    a[FINE - 1] = v_ref[FINE - 1]
    a[FINE + rows] = v_ref[FINE + rows]
    for i in range(2):
        for part in range(2):
            at = pl.ds(TILE + part * half_columns, half_columns)
            k = DEEP + 2 * i + part
            low, high = by_side(even_b, coarse_e[k], coarse_o[k])
            a[1 + i, at, :] = low
            a[FINE + rows + 1 + i, at, :] = high
    end = rows + 2 * FINE
    quarter = end // 4
    first = half_rows

    def fine_lane(k, _):
        low, high = by_side(even_l, coarse_lane_e[first + k], coarse_lane_o[first + k])
        s = sublane(low)
        for g in range(4):
            r = g * quarter + k
            a[r, left, :] = jnp.where(s == TILE - 1, v_ref[r, left, :], roll(low, 5 - 2 * g, 0))
            a[r, right, :] = jnp.where(s == 0, v_ref[r, right, :], roll(high, 1 - 2 * g, 0))
        return 0

    lax.fori_loop(0, quarter, fine_lane, 0, unroll=2)
    at = coarse_lane_e.shape[0] - 1
    low, high = by_side(even_l, coarse_lane_e[at], coarse_lane_o[at])
    for r, turn in ((FINE - 2, 0), (FINE + rows + 1, 4)):
        a[r, left, :] = roll(low, turn, 0)
        a[r, right, :] = roll(high, turn, 0)
    across = columns // 2 + TILE
    skip = TILE - TILE // 2

    def spread_row(k):
        value = source[DEEP - 2 + k, pl.ds(skip, across), :]
        spread[k, pl.ds(0, across, 2), :] = value
        spread[k, pl.ds(1, across, 2), :] = value
        return spread[k]

    for k in (0, 1, half_rows + 2, half_rows + 3):
        both = spread_row(k)
        a[2 * k] += both
        a[2 * k + 1] += both

    def correct(k, _):
        both = spread_row(k)
        ends = [lax.slice_in_dim(both, s, s + TILE, axis=0) for s in (0, TILE + columns)]
        middle = lax.slice_in_dim(both, TILE, TILE + columns, axis=0)
        for part in range(2):
            r = 2 * k + part
            a[r, fine_own, :] = v_ref[r, fine_own, :] + middle
            a[r, left, :] += ends[0]
            a[r, right, :] += ends[1]
        return 0

    lax.fori_loop(2, half_rows + 2, correct, 0, unroll=2)
    sweep(a, b, load, w, 2, end - 2)
    sweep(b, a, load, w, 3, end - 3)
    piece = rows // CHUNKS

    def put(source, hbm, at, sem):
        copy = pltpu.make_async_copy(
            source.at[pl.ds(FINE + at, piece), fine_own, :],
            hbm.at[pl.ds(at, piece), :, layers],
            sem,
        )
        copy.start()
        return copy

    puts = [put(a, u_hbm, c * piece, sems.at[c]) for c in range(CHUNKS)]

    def remains(i, carry):
        up, here = carry
        down = a[FINE + i + 1]
        around = (up + down) + (roll(here, 1, 0) + roll(here, -1, 0))
        value = lax.slice_in_dim(load[FINE + i] + around, TILE, TILE + columns, axis=0)
        mine = lax.slice_in_dim(here, TILE, TILE + columns, axis=0)
        b[FINE + i, fine_own, :] = value - (4.0 + m_own[i]) * mine
        return here, down

    carry = (a[FINE - 1], a[FINE])
    for c in range(CHUNKS):
        carry = lax.fori_loop(c * piece, (c + 1) * piece, remains, carry, unroll=2)
        puts.append(put(b, d_hbm, c * piece, sems.at[CHUNKS + c]))
    for copy in puts:
        copy.wait()


def call(kernel, chain, outs, args, limit, scratch=(), sems=0, hbm=0, hbm_out=False, aliases=None, extra=0, us=1):
    far, near = pl.BlockSpec(memory_space=pltpu.HBM), pl.BlockSpec(memory_space=pltpu.VMEM)
    near_count = len(args) - hbm - extra
    return pl.pallas_call(
        functools.partial(kernel, chain),
        in_specs=[far] * hbm + [near] * near_count + [far] * extra,
        out_specs=[far if hbm_out else near] * len(outs),
        out_shape=[jax.ShapeDtypeStruct(s, jnp.float32) for s in outs],
        scratch_shapes=[pltpu.VMEM(s + (LANES,), jnp.float32) for s in scratch]
        + ([pltpu.SemaphoreType.DMA((sems,))] if sems else []),
        input_output_aliases=aliases or {},
        cost_estimate=pl.CostEstimate(flops=us * COST, bytes_accessed=0, transcendentals=0),
        compiler_params=pltpu.CompilerParams(vmem_limit_bytes=limit * 1024 * 1024),
    )(*args)


def program(f, u, m):
    rows, columns, layers = f.shape
    half_rows, half_columns = rows // 2, columns // 2
    end, total = rows + 2 * FINE, half_rows + 2 * DEEP
    wide, half_wide = columns + 2 * TILE, half_columns + 2 * TILE
    groups = layers // LANES
    block, coarse_block = (rows, columns, LANES), (half_rows, half_columns, LANES)
    chains = range(groups)

    strip, lane = (10, columns, LANES), (rows, TILE, LANES)
    fines, fine_lanes = [], []

    def send(strips):
        fines.append(swap("band", *strips[:2]))
        fine_lanes.append(swap("lane", *strips[2:]))

    first = call(
        first_kernel, 0, ([strip] * 2 + [lane] * 2) * (groups - 1), (u, f, m), FAR,
        scratch=[(groups - 1, 6, rows, TILE)], sems=12 * (groups - 1), hbm=3, us=4,
    )
    for c in range(groups - 1):
        send(first[4 * c : 4 * c + 4])
    *owns, mass, m_e, m_o, n_e, n_o = call(
        load_kernel, 0,
        [block] * 3 * groups + [(groups,) + coarse_block]
        + [(10 + groups * DEEP // 2, columns, LANES)] * 2 + [(rows + groups * half_rows, TILE, LANES)] * 2,
        (u, f, m), LOAD, scratch=[(half_rows, columns)], sems=3 * groups, hbm=3, us=8,
    )
    send((m_e, m_o, n_e, n_o))
    masses, mass_lanes = fines[-1], fine_lanes[-1]
    owns = [owns[3 * c : 3 * c + 3] for c in chains]
    fine_corners, values, loads, coarses, fields = [], [], [], [], []
    for c in chains:
        strips = call(
            fine_corner_kernel, c, [(2 * CORNER, TILE, LANES)] * 2, (*owns[c], *fines[c], *loads), 4
        )
        fine_corners.append(swap("lane", *strips))
        v, load, *strips, load_wide, w_wide = call(
            before_kernel, c,
            [(end, wide, LANES), coarse_block] + [(DEEP + 4, half_columns, LANES)] * 2
            + [(end, wide, LANES)] * 2,
            (*owns[c], *fines[c], *fine_lanes[c], *fine_corners[c]), 10, us=6,
            scratch=[(end, wide)] * 2 + [(half_rows, columns)],
        )
        fields.append((load_wide, w_wide))
        values.append(v)
        loads.append(load)
        coarses.append(swap("band", *strips))
    coarse_lanes = []
    lane_rows = half_rows + end // 4 + 2 * DEEP - 1
    for c in chains:
        strips = call(
            coarse_pack_kernel, c, [(lane_rows, TILE, LANES)] * 2, (loads[c], values[c], *coarses[c], *masses, *loads[c + 1 :]), 4
        )
        coarse_lanes.append(swap("lane", *strips))
    xs, nexts = [], []
    for c in chains:
        x, *strips, load_wide, w_wide = call(
            coarse_kernel, c,
            [coarse_block] + [(SECOND, half_columns, LANES)] * 2 + [(total, half_wide, LANES)] * 2,
            (loads[c], mass, *coarses[c], *masses, *coarse_lanes[c], *mass_lanes), 6, us=4,
            scratch=[(total, half_wide)] * 2,
        )
        fields[c] += (load_wide, w_wide)
        xs.append(x)
        nexts.append(swap("band", *strips))
    next_lanes = []
    for c in chains:
        strips = call(
            value_pack_kernel, c, [(half_rows + DEEP - 1, TILE, LANES)] * 2, (xs[c], *nexts[c], *xs[c + 1 :]), 4
        )
        next_lanes.append(swap("lane", *strips))
    results = ()
    for c in chains:
        args = (
            owns[c][2], values[c], xs[c], *fields[c], *coarses[c], *coarse_lanes[c], *nexts[c], *next_lanes[c],
        )
        results = tuple(
            call(
                after_kernel, c, [(rows, columns, layers)] * 2, args + results, 12, us=8,
                scratch=[(end, wide)] * 2 + [(total, half_wide)] * 2 + [(half_rows + 4, wide)],
                sems=2 * CHUNKS, hbm_out=True, extra=len(results),
                aliases={len(args) + k: k for k in range(len(results))},
            )
        )
    return results


def solution(mesh):
    return jax.shard_map(
        program,
        mesh=mesh,
        in_specs=(P("band", "lane", None), P("band", "lane", None), P("band", "lane", None)),
        out_specs=(P("band", "lane", None), P("band", "lane", None)),
        check_vma=False,
    )
```
